32 devices in a mesh: rep: 1 (over z), dp: 32 (over x, y, core).
Axes of the slice: x: 4, y: 4, z: 1, core: 2. Of those that a mesh axis runs over, the one named last changes fastest.
The devices are a block of a 4x4x8 slice.
Arguments:
- x: bfloat16 [32, 2048, 640], P(('rep', 'dp'))
- dy: bfloat16 [32, 2048, 640], P(('rep', 'dp'))
- w_gate: bfloat16 [2, 640, 3456], replicated
- w_up: bfloat16 [2, 640, 3456], replicated
- w_down: bfloat16 [2, 3456, 640], replicated
- m_w_gate: float32 [2, 640, 3456], replicated
- m_w_up: float32 [2, 640, 3456], replicated
- m_w_down: float32 [2, 3456, 640], replicated
- v_w_gate: float32 [2, 640, 3456], replicated
- v_w_up: float32 [2, 640, 3456], replicated
- v_w_down: float32 [2, 3456, 640], replicated
Outputs:
- output 1: bfloat16 [2, 640, 3456], P('rep')
- output 2: bfloat16 [2, 640, 3456], P('rep')
- output 3: bfloat16 [2, 3456, 640], P('rep')
- output 4: float32 [2, 640, 3456], P('rep')
- output 5: float32 [2, 640, 3456], P('rep')
- output 6: float32 [2, 3456, 640], P('rep')
- output 7: float32 [2, 640, 3456], P('rep')
- output 8: float32 [2, 640, 3456], P('rep')
- output 9: float32 [2, 3456, 640], P('rep')
All inputs are finite; a program needn't handle non-finite values.
Results may differ from the reference program's by a relative error of at most 0.022.
Values are sent between devices in bfloat16 or wider.
A program may use at most 768 MiB of HBM per device.

```python
import jax
import jax.numpy as jnp
from jax import lax

SEQUENCES = 32
TOKENS = 2048
D = 640
FF = 3456
LAYERS = 2
NAMES = ("w_gate", "w_up", "w_down")
SHAPES = {"w_gate": (LAYERS, D, FF), "w_up": (LAYERS, D, FF), "w_down": (LAYERS, FF, D)}


def bump(key, n, height):
    away = (jnp.arange(n, dtype=jnp.int32) - jax.random.randint(key, (), 0, n, jnp.int32)) % n
    return jnp.where(away < n // 8, height, 1.0)


def together(key, own, strength):
    shared = jax.random.normal(key, own.shape[1:], jnp.float32)
    return (own + strength * shared) * lax.rsqrt(1 + strength * strength)


def setup_inputs(seed: int = 0, part: int = 0) -> dict:
    kx, kdy, ka, kb, kz, kf, kh, kl, *keys = jax.random.split(jax.random.key(seed), 8 + 3 * len(NAMES))
    kx, kdy, ka, kb = (jax.random.fold_in(k, part) for k in (kx, kdy, ka, kb))
    kw, km, kv = (keys[i::3] for i in range(3))
    shape = (SEQUENCES, TOKENS, D)
    much_x, much_dy = jax.random.uniform(kz, (2,), jnp.float32, 0.0, 1.0)
    loud = 2.0 ** jax.random.uniform(jax.random.fold_in(kz, 1), (), jnp.float32, -1.0, 2.0)
    layers = 2.0 ** jax.random.uniform(kl, (LAYERS, 1, 1), jnp.float32, -1.0, 1.0)
    x = together(ka, jax.random.normal(kx, shape, jnp.float32), much_x) * bump(kf, D, 4.0)
    dy = together(kb, jax.random.normal(kdy, shape, jnp.float32), much_dy)
    drawn = {"x": x.astype(jnp.bfloat16), "dy": (loud * dy * (SEQUENCES * TOKENS) ** -0.5).astype(jnp.bfloat16)}
    for key, name in zip(kw, NAMES, strict=True):
        w = jax.random.normal(key, SHAPES[name], jnp.float32) * SHAPES[name][1] ** -0.5
        drawn[name] = (w * {"w_gate": 1.0, "w_up": bump(kh, FF, 4.0), "w_down": layers}[name]).astype(jnp.bfloat16)
    for key, name in zip(km, NAMES, strict=True):
        drawn[f"m_{name}"] = 0.1 * jax.random.normal(key, SHAPES[name], jnp.float32)
    for key, name in zip(kv, NAMES, strict=True):
        drawn[f"v_{name}"] = jax.random.uniform(key, SHAPES[name], jnp.float32, 0.005, 0.015)
    return drawn


def matmul(a, w):
    return jnp.dot(a, w, preferred_element_type=jnp.float32).astype(jnp.bfloat16)


def normed(h):
    wide = h.astype(jnp.float32)
    scale = lax.rsqrt(jnp.mean(wide**2, -1, keepdims=True) + 1e-6)
    return (wide * scale).astype(jnp.bfloat16)


def layer(h, w):
    a = normed(h)
    gate = jnp.dot(a, w["w_gate"], preferred_element_type=jnp.float32)
    up = jnp.dot(a, w["w_up"], preferred_element_type=jnp.float32)
    return h + matmul((jax.nn.silu(gate) * up).astype(jnp.bfloat16), w["w_down"])


def adamw(w, m, v, g):
    m = 0.9 * m + 0.1 * g
    v = 0.95 * v + 0.05 * g * g
    step = m * lax.rsqrt(v + 1e-8) + 0.1 * w
    return (w - 0.02 * step).astype(jnp.bfloat16), m, v


def clipped(gradients, sum_of_squares, count):
    factor = jnp.minimum(1.0, 0.5 * lax.rsqrt(sum_of_squares / count + 1e-30))
    return [g * factor for g in gradients]


def stack(weights, h):
    return lax.scan(lambda h, w: (layer(h, w), None), h, weights)[0]


def reference(x, dy, w_gate, w_up, w_down, m_w_gate, m_w_up, m_w_down, v_w_gate, v_w_up, v_w_down):
    weights = dict(zip(NAMES, (w_gate, w_up, w_down), strict=True))

    def take(so_far, sequence):
        h, by_y = sequence
        _, back = jax.vjp(lambda w: stack(w, h), weights)
        return jax.tree.map(lambda total, term: total + term.astype(jnp.float32), so_far, back(by_y)[0]), None

    none_yet = {name: jnp.zeros(w.shape, jnp.float32) for name, w in weights.items()}
    by_weights, _ = lax.scan(take, none_yet, (x, dy))
    gradients = [by_weights[name].astype(jnp.bfloat16).astype(jnp.float32) for name in NAMES]
    gradients = clipped(gradients, sum(jnp.sum(g * g) for g in gradients), sum(g.size for g in gradients))
    new = [
        adamw(w.astype(jnp.float32), m, v, g)
        for w, m, v, g in zip((w_gate, w_up, w_down), (m_w_gate, m_w_up, m_w_down), (v_w_gate, v_w_up, v_w_down), gradients, strict=True)
    ]
    return tuple(one[which] for which in range(3) for one in new)
```

```python
import functools
import math

import jax
import jax.numpy as jnp
from jax import lax
from jax.experimental import pallas as pl
from jax.experimental.pallas import tpu as pltpu
from jax.sharding import PartitionSpec as P


F32, BF16 = jnp.float32, jnp.bfloat16
LANES = 128
VMEM_BYTES = 67_043_328
STREAMS = 4
STEPS = 4


def cut(n, size):
    return [(at, min(size, n - at)) for at in range(0, n, size)]


def normed(h):
    wide = h.astype(F32)
    scale = lax.rsqrt(jnp.mean(wide * wide, -1, keepdims=True) + 1e-6)
    return wide, scale


def gated(gate, up):
    sig = 0.5 * jnp.tanh(0.5 * gate) + 0.5
    silu = gate * sig
    return silu, up * (sig + silu * (1.0 - sig))


def dot(a, b):
    return jnp.dot(a, b, preferred_element_type=F32)


def dot_t(a, b):
    return lax.dot_general(a, b, (((1,), (1,)), ((), ())), preferred_element_type=F32)


def tokens_kernel(width, x_ref, dy_ref, wg_ref, wu_ref, wd_ref, hid, dg, du, sd, sa, silu_ref, slope_ref):
    ff, padded = wg_ref.shape[2], hid.shape[2]
    columns = [slice(at, at + n) for at, n in cut(ff, width)]
    for ref in (hid, dg, du):
        ref[:, :, ff:] = jnp.zeros((2, ref.shape[1], padded - ff), BF16)
    h = x_ref[...]
    wide, scale = normed(h)
    a = (wide * scale).astype(BF16)
    sa[1] = a
    for c in columns:
        gate, up = dot(a, wg_ref[0, :, c]), dot(a, wu_ref[0, :, c])
        silu, slope = gated(gate, up)
        hid[1, :, c] = (silu * up).astype(BF16)
        silu_ref[:, c] = silu
        slope_ref[:, c] = slope
    h = h + dot(hid[1, :, :ff], wd_ref[0]).astype(BF16)
    wide, scale = normed(h)
    a = (wide * scale).astype(BF16)
    sa[0] = a
    dy = dy_ref[...]
    sd[0] = dy
    for c in columns:
        gate, up = dot(a, wg_ref[1, :, c]), dot(a, wu_ref[1, :, c])
        silu, slope = gated(gate, up)
        hid[0, :, c] = (silu * up).astype(BF16)
        by_hid = dot_t(dy, wd_ref[1, c, :]).astype(BF16).astype(F32)
        dg[0, :, c] = (by_hid * slope).astype(BF16)
        du[0, :, c] = (by_hid * silu).astype(BF16)
    by_a = (dot_t(dg[0, :, :ff], wg_ref[1]).astype(BF16) + dot_t(du[0, :, :ff], wu_ref[1]).astype(BF16)).astype(F32)
    along = jnp.sum(by_a * wide, -1, keepdims=True) * (1.0 / wide.shape[-1])
    by_h = dy + (scale * by_a - (scale * scale * scale * along) * wide).astype(BF16)
    sd[1] = by_h
    for c in columns:
        by_hid = dot_t(by_h, wd_ref[0, c, :]).astype(BF16).astype(F32)
        dg[1, :, c] = (by_hid * slope_ref[:, c]).astype(BF16)
        du[1, :, c] = (by_hid * silu_ref[:, c]).astype(BF16)


def tokens_part(x, dy, wg, wu, wd, padded, rows=256, width=768):
    t, d = x.shape
    ff = wg.shape[2]
    tok = pl.BlockSpec((rows, d), lambda i: (i, 0))
    whole = lambda w: pl.BlockSpec(w.shape, lambda i: (0, 0, 0), pipeline_mode=pl.Buffered(1))
    out = lambda n: pl.BlockSpec((2, rows, n), lambda i: (0, i, 0))
    return pl.pallas_call(
        functools.partial(tokens_kernel, width),
        grid=(t // rows,),
        in_specs=[tok, tok, whole(wg), whole(wu), whole(wd)],
        out_specs=[out(padded)] * 3 + [out(d)] * 2,
        out_shape=[jax.ShapeDtypeStruct((2, t, padded), BF16)] * 3 + [jax.ShapeDtypeStruct((2, t, d), BF16)] * 2,
        scratch_shapes=[pltpu.VMEM((rows, ff), F32)] * 2,
        compiler_params=pltpu.CompilerParams(vmem_limit_bytes=VMEM_BYTES),
        cost_estimate=pl.CostEstimate(flops=18 * t * d * ff, bytes_accessed=20 * t * ff, transcendentals=2 * t * ff),
        name="tokens",
    )(x, dy, wg, wu, wd)


def bits(p):
    return (p + p // 2) % 2, p // 2


def other(p, which):
    return p + 1 - 2 * (p % 2) if which == 0 else 3 - p


def place(me, side):
    core, chip = me % 2, me // 2
    x, y = chip // side, chip % side
    return core, x + core * (y - x), y + core * (x - y)


def device(core, first, second, side):
    x, y = first + core * (second - first), second + core * (first - second)
    return (x * side + y) * 2 + core


def stream_bits(first, second, slot):
    f, s = bits(first), bits(second)
    return (f[slot], f[1 - slot], s[slot], s[1 - slot])


def stream_partner(core, first, second, slot, step, side):
    which = slot if step % 2 == 0 else 1 - slot
    if step < 2:
        return device(core, other(first, which), second, side)
    return device(core, first, other(second, which), side)


def grads_kernel(side, chunks, hid, dg, du, sd, sa, own0, own1, sib0, sib1, squares, *scratch):
    (bbuf, sdbuf, sabuf, bsem, ssem, acc_d, acc_u, to_d, to_u, from_d, from_u, *rest) = scratch
    sends_d, sends_u, gets_d, gets_u = rest[0:4], rest[4:8], rest[8:12], rest[12:16]
    (gather, sq_acc, sq_send, sq_get, tosem, fromsem, sendsem, getsem, agsend, agget, sqs, sqg, outsem) = rest[16:]
    big = (hid, dg, du)
    half_width = sum(n for _, n in chunks)
    me = lax.axis_index("dp")
    core, first, second = place(me, side)
    sibling = me + 1 - 2 * core
    slot_bits = [stream_bits(first, second, j) for j in range(2)]
    partner = [[stream_partner(core, first, second, j, k, side) for k in range(STEPS)] for j in range(2)]

    barrier = pltpu.get_barrier_semaphore()
    neighbours = (sibling, partner[0][0], partner[0][1], partner[0][2], partner[0][3])
    for to in neighbours:
        pl.semaphore_signal(barrier, inc=1, device_id={"dp": to}, device_id_type=pl.DeviceIdType.MESH)
    pl.semaphore_wait(barrier, len(neighbours))

    def remote(src, dst, send, get, to):
        return pltpu.make_async_remote_copy(
            src_ref=src, dst_ref=dst, send_sem=send, recv_sem=get, device_id={"dp": to}, device_id_type=pl.DeviceIdType.MESH
        )

    acc = lambda p: acc_d if p == 0 else acc_u.at[p - 1]
    to_buf = lambda p: to_d if p == 0 else to_u
    from_buf = lambda p: from_d if p == 0 else from_u.at[p - 1]
    send_buf = lambda p, k, j: (sends_d[k].at[j] if p == 0 else sends_u[k].at[p - 1, j])
    get_buf = lambda p, k, j: (gets_d[k].at[j] if p == 0 else gets_u[k].at[p - 1, j])
    height = lambda p: (acc_d if p == 0 else acc_u).shape[-2]
    across = lambda p: remote(to_buf(p), from_buf(p), tosem.at[p], fromsem.at[p], sibling)
    hop = lambda p, k, j: remote(
        send_buf(p, k, j), get_buf(p, k, j), sendsem.at[p, k, j], getsem.at[p, k, j], partner[j][k]
    )

    def kept(p, j, k):
        return sum((slot_bits[j][i] * (height(p) >> (i + 1)) for i in range(k)), 0)

    def rows(at, n):
        return pl.ds(pl.multiple_of(at, 8), n)

    def give(p, j, k, arrived):
        n = height(p) >> (k + 1)
        start, bit = kept(p, j, k), slot_bits[j][k]
        going, staying = (1 - bit) * n, bit * n
        buf = send_buf(p, k, j)
        total = acc(p)[j, rows(start + going, n), :] + arrived(1 - bit, n).astype(F32)
        if k == 2:
            buf[0], buf[1] = total[: n // 2].astype(BF16), total[n // 2 :].astype(BF16)
        else:
            buf[...] = total.astype(BF16)
        hop(p, k, j).start()
        acc(p)[j, rows(start + staying, n), :] += arrived(bit, n).astype(F32)

    def ev0(p, _):
        across(p).start()

    def ev1(p, _):
        across(p).wait()
        for j in range(2):
            give(p, j, 0, lambda which, n, j=j: from_buf(p)[j, pl.ds(pl.multiple_of(which * n, 16), n), :])

    def ev2(p, _):
        for j in range(2):
            hop(p, 0, j).wait()
            give(p, j, 1, lambda which, n, j=j: get_buf(p, 0, j)[pl.ds(pl.multiple_of(which * n, 16), n), :])

    def ev3(p, _):
        for j in range(2):
            hop(p, 1, j).wait()
            give(p, j, 2, lambda which, n, j=j: get_buf(p, 1, j)[pl.ds(pl.multiple_of(which * n, 16), n), :])

    def ev4(p, _):
        for j in range(2):
            hop(p, 2, j).wait()
            give(p, j, 3, lambda which, n, j=j: get_buf(p, 2, j)[which])

    def ev5(p, layer):
        for j in range(2):
            hop(p, 3, j).wait()
            n = height(p) >> STEPS
            total = acc(p)[j, rows(kept(p, j, STEPS), n), :] + get_buf(p, 3, j)[...].astype(F32)
            flat = jnp.concatenate([total[:, c : c + LANES] for c in range(0, total.shape[1], LANES)], axis=0)
            flat = flat.astype(BF16)
            gather[j, 2 * slot_bits[j][2] + slot_bits[j][3], 3 * layer + p] = flat
            wide = flat.astype(F32)
            sq_acc[...] += jnp.sum((wide * wide).reshape(-1, 8, LANES), axis=0)

    def fetch(p, layer, q):
        at, n = chunks[q % 2]
        side_of = 1 - core if q < 2 else core
        col = pl.ds(pl.multiple_of(side_of * half_width + at, LANES), n)
        return pltpu.make_async_copy(big[p].at[layer, :, col], bbuf.at[q % 2, :, pl.ds(0, n)], bsem.at[q % 2])

    def fetch_small(p, layer):
        src, dst = (sd, sdbuf) if p == 0 else (sa, sabuf)
        return pltpu.make_async_copy(src.at[layer], dst, ssem.at[0 if p == 0 else 1])

    def product(p, q):
        _, n = chunks[q % 2]
        b = bbuf[q % 2, :, :n]
        over_tokens = (((0,), (0,)), ((), ()))
        if p == 0:
            return lax.dot_general(b, sdbuf[...], over_tokens, preferred_element_type=F32)
        return lax.dot_general(sabuf[...], b, over_tokens, preferred_element_type=F32)

    def put(p, q, value):
        at, n = chunks[q % 2]
        length = half_width // 2
        ref = to_buf(p) if q < 2 else acc(p)
        for j in range(2):
            lo, hi = max(at, j * length), min(at + n, (j + 1) * length)
            if lo < hi:
                if p == 0:
                    ref[j, lo - j * length : hi - j * length, :] = value[lo - at : hi - at, :].astype(ref.dtype)
                else:
                    ref[j, :, lo - j * length : hi - j * length] = value[:, lo - at : hi - at].astype(ref.dtype)

    layers = 2
    sq_acc[...] = jnp.zeros_like(sq_acc)
    fetch_small(0, 0).start()
    fetch(0, 0, 0).start()
    fetch_small(1, 0).start()

    def turn(layer, _):
        def event(fn, p, back):
            before = p - back
            if before >= 0:
                pl.when(layer < layers)(lambda: fn(before, layer))
            else:
                pl.when(layer >= 1)(lambda: fn(before % 3, layer - 1))

        for p in range(3):
            for half in range(2):

                @pl.when(layer < layers)
                def _():
                    if half == 0 and p < 2:
                        fetch_small(p, layer).wait()
                    for q in (2 * half, 2 * half + 1):
                        fetch(p, layer, q).wait()
                        if q < 3:
                            fetch(p, layer, q + 1).start()
                        elif p < 2:
                            fetch(p + 1, layer, 0).start()
                        else:
                            pl.when(layer + 1 < layers)(lambda: fetch(0, layer + 1, 0).start())
                        put(p, q, product(p, q))
                    if half == 1 and p == 0:
                        pl.when(layer + 1 < layers)(lambda: fetch_small(0, layer + 1).start())
                    if half == 1 and p == 2:
                        pl.when(layer + 1 < layers)(lambda: fetch_small(1, layer + 1).start())

                if half == 0:
                    event(ev5, p, 3)
                    event(ev3, p, 2)
                    event(ev0, p, 0)
                else:
                    event(ev4, p, 2)
                    event(ev2, p, 1)
                    event(ev1, p, 0)
        return 0

    lax.fori_loop(0, layers + 1, turn, 0)

    def block(j, at, n):
        return gather.at[j, pl.ds(at, n)]

    def pass_on(step, j):
        b = slot_bits[j]
        at = 2 * b[2] + b[3] if step == 0 else 2 * b[2]
        ref = block(j, at, 1 + step)
        return remote(ref, ref, agsend.at[step, j], agget.at[step, j], partner[j][3 - step])

    def count(step):
        to = partner[0][step] if step < STEPS else sibling
        return remote(sq_send.at[step], sq_get.at[step], sqs.at[step], sqg.at[step], to)

    def count_start(step):
        sq_send[step] = sq_acc[...]
        count(step).start()

    def count_end(step):
        count(step).wait()
        sq_acc[...] += sq_get[step]

    count_start(0)
    for j in range(2):
        pass_on(0, j).start()
    count_end(0)
    count_start(1)
    for j in range(2):
        pass_on(0, j).wait()
        pass_on(1, j).start()
    for step in range(1, STEPS + 1):
        count_end(step)
        if step < STEPS:
            count_start(step + 1)
    squares[...] = sq_acc[...]
    sib = (sib0, sib1)
    own = (own0, own1)

    def over(j):
        return remote(gather.at[j], sib[j], agsend.at[2, j], agget.at[2, j], sibling)

    def out(j):
        return pltpu.make_async_copy(gather.at[j], own[j], outsem.at[j])

    for j in range(2):
        pass_on(1, j).wait()
        out(j).start()
        over(j).start()
    for j in range(2):
        out(j).wait()
        over(j).wait()


def grads_part(hid, dg, du, sd, sa, side, collective_id=1):
    _, t, padded = hid.shape
    d = sd.shape[2]
    half, length = padded // 2, padded // STREAMS
    chunks = [(0, 1024), (1024, half - 1024)] if half > 1024 else cut(half, half // 2)
    widest = max(n for _, n in chunks)
    shard = d * length // (side * side * LANES)
    down, up = (2, length, d), (2, 2, d, length)

    def step_bufs(n_rows, n_cols, lead):
        shapes = []
        for k in range(STEPS):
            n = n_rows >> (k + 1)
            shapes.append((*lead, 2, n // 2, n_cols) if k == 2 else (*lead, n, n_cols))
        return [pltpu.VMEM(s, BF16) for s in shapes]

    steps_d, steps_u = step_bufs(length, d, (2,)), step_bufs(d, length, (2, 2))
    dma = pltpu.SemaphoreType.DMA
    quarter = jax.ShapeDtypeStruct((side, 6, shard, LANES), BF16)
    hbm = pl.BlockSpec(memory_space=pl.ANY)
    return pl.pallas_call(
        functools.partial(grads_kernel, side, chunks),
        in_specs=[hbm] * 5,
        out_specs=[hbm] * 4 + [pl.BlockSpec(memory_space=pltpu.VMEM)],
        out_shape=[quarter] * 4 + [jax.ShapeDtypeStruct((8, LANES), F32)],
        scratch_shapes=[
            pltpu.VMEM((2, t, widest), BF16),
            pltpu.VMEM((t, d), BF16),
            pltpu.VMEM((t, d), BF16),
            dma((2,)),
            dma((2,)),
            pltpu.VMEM(down, F32),
            pltpu.VMEM(up, F32),
            pltpu.VMEM(down, BF16),
            pltpu.VMEM(up[1:], BF16),
            pltpu.VMEM(down, BF16),
            pltpu.VMEM(up, BF16),
            *steps_d,
            *steps_u,
            *steps_d,
            *steps_u,
            pltpu.VMEM((2, side, 6, shard, LANES), BF16),
            pltpu.VMEM((8, LANES), F32),
            pltpu.VMEM((STEPS + 1, 8, LANES), F32),
            pltpu.VMEM((STEPS + 1, 8, LANES), F32),
            dma((3,)),
            dma((3,)),
            dma((3, STEPS, 2)),
            dma((3, STEPS, 2)),
            dma((3, 2)),
            dma((3, 2)),
            dma((STEPS + 1,)),
            dma((STEPS + 1,)),
            dma((2,)),
        ],
        compiler_params=pltpu.CompilerParams(vmem_limit_bytes=VMEM_BYTES, collective_id=collective_id, has_side_effects=True),
        cost_estimate=pl.CostEstimate(flops=12 * t * d * padded, bytes_accessed=6 * t * padded * 2, transcendentals=0),
        name="grads",
    )(hid, dg, du, sd, sa)


def update_kernel(total, shards, n_gs, n_in, places, *refs):
    gs, squares, refs = refs[:n_gs], refs[n_gs], refs[n_gs + 1 :]
    refs = refs[:9] + refs[n_in:]
    wg, wu, wd, mg, mu, md, vg, vu, vd, nwg, nwu, nwd, nmg, nmu, nmd, nvg, nvu, nvd, wide = refs
    source = pl.program_id(0)
    for i, g in enumerate(gs):

        @pl.when(source == i)
        def _():
            wide[...] = g[...].astype(F32)

    mean = jnp.sum(squares[...], keepdims=True) * (1.0 / total)
    factor = jnp.minimum(1.0, 0.5 * lax.rsqrt(mean + 1e-30))

    def one(w, m, v, nw, nm, nv, which):
        n = m.shape[1] // shards
        for b in range(0, shards, 2):
            for c in range(0, m.shape[2], LANES):
                at = c // LANES * n
                g = jnp.concatenate([wide[b, which, at : at + n, :], wide[b + 1, which, at : at + n, :]], axis=0) * factor
                here = (0, slice(b * n, (b + 2) * n), slice(c, c + LANES))
                new_m = 0.9 * m[here] + 0.1 * g
                new_v = 0.95 * v[here] + 0.05 * g * g
                old = w[here].astype(F32)
                nm[here] = new_m
                nv[here] = new_v
                nw[here] = (old - 0.02 * (new_m * lax.rsqrt(new_v + 1e-8) + 0.1 * old)).astype(BF16)

    one(wd, md, vd, nwd, nmd, nvd, 0)
    one(wg, mg, vg, nwg, nmg, nvg, 1)
    one(wu, mu, vu, nwu, nmu, nvu, 2)


def update_part(places, gs, squares, old, so_far):
    shards, _, shard, _ = gs[0].shape
    layers, d, ff = old[0].shape
    length = shard * shards * shards * LANES // d
    total = 3.0 * layers * d * ff
    g_spec = lambda i: pl.BlockSpec((shards, 3, shard, LANES), lambda s, l, at: (0, jnp.clip((s - i) * layers + l, 0, layers - 1), 0, 0))
    up_spec = pl.BlockSpec((1, d // shards, length), lambda s, l, at: (layers - 1 - l, at[1, s], at[0, s]))
    down_spec = pl.BlockSpec((1, length // shards, d), lambda s, l, at: (layers - 1 - l, at[0, s] * shards + at[1, s], 0))
    nine = [up_spec, up_spec, down_spec] * 3
    hbm = pl.BlockSpec(memory_space=pl.ANY)
    n_alias = len(so_far)
    return pl.pallas_call(
        functools.partial(update_kernel, total, shards, len(gs), 9 + n_alias),
        grid_spec=pltpu.PrefetchScalarGridSpec(
            num_scalar_prefetch=1,
            grid=(len(gs), layers),
            in_specs=[*(g_spec(i) for i in range(len(gs))), pl.BlockSpec((8, LANES), lambda s, l, at: (0, 0)), *nine, *[hbm] * n_alias],
            out_specs=nine,
            scratch_shapes=[pltpu.VMEM((shards, 3, shard, LANES), F32)],
        ),
        out_shape=[jax.ShapeDtypeStruct(a.shape, a.dtype) for a in old],
        input_output_aliases={1 + len(gs) + 1 + 9 + i: i for i in range(n_alias)},
        compiler_params=pltpu.CompilerParams(vmem_limit_bytes=VMEM_BYTES),
        cost_estimate=pl.CostEstimate(flops=30 * 3 * layers * d * ff, bytes_accessed=5 * 3 * layers * d * ff, transcendentals=0),
        name="update",
    )(places, *gs, squares, *old, *so_far)


def solution(mesh):
    group = mesh.shape["dp"]
    side = math.isqrt(group // 2)
    assert side == 4 and 2 * side * side == group

    def pairs(slot, step):
        found = []
        for me in range(group):
            core, first, second = place(me, side)
            found.append((me, stream_partner(core, first, second, slot, step, side)))
        return found

    siblings = [(me, me + 1 - 2 * (me % 2)) for me in range(group)]

    def step(x, dy, *arrays):
        wg, wu, wd = arrays[:3]
        ff = wg.shape[2]
        padded = -(-ff // (STREAMS * LANES)) * STREAMS * LANES
        hid, dg, du, sd, sa = tokens_part(x[0], dy[0], wg, wu, wd, padded)
        own0, own1, sib0, sib1, squares = grads_part(hid, dg, du, sd, sa, side)

        me = lax.axis_index("dp")
        core, first, second = place(me, side)

        def along(arrays, step):
            return [lax.ppermute(a, "dp", pairs(j, step)) for j, a in enumerate(arrays)]

        def across(arrays):
            return [lax.ppermute(a, "dp", siblings) for a in arrays]

        def stand(theirs, flip):
            found = []
            for j in range(2):
                b = stream_bits(second, first, j) if theirs else stream_bits(first, second, j)
                b = [1 - bit if turned else bit for bit, turned in zip(b[:2], flip)]
                found.append((2 * (1 - core if theirs else core) + j, 2 * b[0] + b[1]))
            return found

        def update(new, *parts):
            where = [one for _, theirs, flip in parts for one in stand(theirs, flip)]
            places = jnp.stack([jnp.stack([at[i] for at in where]) for i in range(2)]).astype(jnp.int32)
            return update_part(places, [g for gs, _, _ in parts for g in gs], squares, arrays, new)

        own, sib = [own0, own1], [sib0, sib1]
        second_bit, first_bit, both = (0, 1), (1, 0), (1, 1)
        third, fourth = along(own, 1), along(own, 0)
        new = update((), (own, False, (0, 0)), (sib, True, (0, 0)))
        third, new = lax.optimization_barrier((third, new))
        fifth, third_too = along(third, 0), across(third)
        new = update(new, (third, False, second_bit))
        fourth, third_too, new = lax.optimization_barrier((fourth, third_too, new))
        fourth_too = across(fourth)
        new = update(new, (third_too, True, second_bit), (fourth, False, first_bit))
        fifth, fourth_too, new = lax.optimization_barrier((fifth, fourth_too, new))
        fifth_too = across(fifth)
        new = update(new, (fourth_too, True, first_bit), (fifth, False, both))
        fifth_too, new = lax.optimization_barrier((fifth_too, new))
        new = update(new, (fifth_too, True, both))
        return tuple(new)

    return jax.shard_map(
        step,
        mesh=mesh,
        in_specs=(P(("rep", "dp"), None, None),) * 2 + (P(None, None, None),) * 9,
        out_specs=(P("rep", None, None),) * 9,
        check_vma=False,
    )
```

```python
import functools
import math

import jax
import jax.numpy as jnp
import numpy as np
from jax import lax
from jax.experimental import pallas as pl
from jax.experimental.pallas import tpu as pltpu
from jax.sharding import PartitionSpec as P


F32, BF16 = jnp.float32, jnp.bfloat16
LANES = 128
VMEM_BYTES = 67_043_328
STREAMS = 4
STEPS = 4


def cut(n, size):
    return [(at, min(size, n - at)) for at in range(0, n, size)]


def normed(h):
    wide = h.astype(F32)
    scale = lax.rsqrt(jnp.mean(wide * wide, -1, keepdims=True) + 1e-6)
    return wide, scale


def gated(gate, up):
    sig = 0.5 * jnp.tanh(0.5 * gate) + 0.5
    silu = gate * sig
    return silu, up * (sig + silu * (1.0 - sig))


def dot(a, b):
    return jnp.dot(a, b, preferred_element_type=F32)


def dot_t(a, b):
    return lax.dot_general(a, b, (((1,), (1,)), ((), ())), preferred_element_type=F32)


def tokens_kernel(width, x_ref, dy_ref, wg_ref, wu_ref, wd_ref, hid, dgu, sd, sa, silu_ref, slope_ref):
    ff, padded = wg_ref.shape[2], hid.shape[2]
    columns = [slice(at, at + n) for at, n in cut(ff, width)]
    hid[:, :, ff:] = jnp.zeros((2, hid.shape[1], padded - ff), BF16)
    dgu[:, :, :, ff:] = jnp.zeros((2, 2, hid.shape[1], padded - ff), BF16)
    h = x_ref[...]
    wide, scale = normed(h)
    a = (wide * scale).astype(BF16)
    sa[1] = a
    for c in columns:
        gate, up = dot(a, wg_ref[0, :, c]), dot(a, wu_ref[0, :, c])
        silu, slope = gated(gate, up)
        hid[1, :, c] = (silu * up).astype(BF16)
        silu_ref[:, c] = silu
        slope_ref[:, c] = slope
    h = h + dot(hid[1, :, :ff], wd_ref[0]).astype(BF16)
    wide, scale = normed(h)
    a = (wide * scale).astype(BF16)
    sa[0] = a
    dy = dy_ref[...]
    sd[0] = dy
    for c in columns:
        gate, up = dot(a, wg_ref[1, :, c]), dot(a, wu_ref[1, :, c])
        silu, slope = gated(gate, up)
        hid[0, :, c] = (silu * up).astype(BF16)
        by_hid = dot_t(dy, wd_ref[1, c, :]).astype(BF16).astype(F32)
        dgu[0, 0, :, c] = (by_hid * slope).astype(BF16)
        dgu[0, 1, :, c] = (by_hid * silu).astype(BF16)
    by_a = dot_t(wg_ref[1], dgu[0, 0, :, :ff]).astype(BF16) + dot_t(wu_ref[1], dgu[0, 1, :, :ff]).astype(BF16)
    by_a = by_a.astype(F32).T
    along = jnp.sum(by_a * wide, -1, keepdims=True) * (1.0 / wide.shape[-1])
    by_h = dy + (scale * by_a - (scale * scale * scale * along) * wide).astype(BF16)
    sd[1] = by_h
    for c in columns:
        by_hid = dot_t(by_h, wd_ref[0, c, :]).astype(BF16).astype(F32)
        dgu[1, 0, :, c] = (by_hid * slope_ref[:, c]).astype(BF16)
        dgu[1, 1, :, c] = (by_hid * silu_ref[:, c]).astype(BF16)


def tokens_part(x, dy, wg, wu, wd, padded, rows=256, width=256):
    t, d = x.shape
    ff = wg.shape[2]
    tok = pl.BlockSpec((rows, d), lambda i: (i, 0))
    whole = lambda w: pl.BlockSpec(w.shape, lambda i: (0, 0, 0), pipeline_mode=pl.Buffered(1))
    out = lambda n: pl.BlockSpec((2, rows, n), lambda i: (0, i, 0))
    return pl.pallas_call(
        functools.partial(tokens_kernel, width),
        grid=(t // rows,),
        in_specs=[tok, tok, whole(wg), whole(wu), whole(wd)],
        out_specs=[out(padded), pl.BlockSpec((2, 2, rows, padded), lambda i: (0, 0, i, 0)), out(d), out(d)],
        out_shape=[
            jax.ShapeDtypeStruct((2, t, padded), BF16),
            jax.ShapeDtypeStruct((2, 2, t, padded), BF16),
            *[jax.ShapeDtypeStruct((2, t, d), BF16)] * 2,
        ],
        scratch_shapes=[pltpu.VMEM((rows, ff), F32)] * 2,
        compiler_params=pltpu.CompilerParams(vmem_limit_bytes=VMEM_BYTES),
        cost_estimate=pl.CostEstimate(flops=18 * t * d * ff, bytes_accessed=20 * t * ff, transcendentals=2 * t * ff),
        name="tokens",
    )(x, dy, wg, wu, wd)


def bits(p):
    return (p + p // 2) % 2, p // 2


def other(p, which):
    return p + 1 - 2 * (p % 2) if which == 0 else 3 - p


def place(me, side):
    core, chip = me % 2, me // 2
    x, y = chip // side, chip % side
    return core, x + core * (y - x), y + core * (x - y)


def device(core, first, second, side):
    x, y = first + core * (second - first), second + core * (first - second)
    return (x * side + y) * 2 + core


def stream_bits(first, second, slot):
    f, s = bits(first), bits(second)
    return (f[slot], f[1 - slot], s[slot], s[1 - slot])


def stream_partner(core, first, second, slot, step, side):
    which = slot if step % 2 == 0 else 1 - slot
    if step < 2:
        return device(core, other(first, which), second, side)
    return device(core, first, other(second, which), side)


def grads_kernel(side, devices, chunks, hid, dgu, sd, sa, own0, own1, sib0, sib1, squares, *scratch):
    bbuf, sdbuf, sabuf, acc, to, came, *rest = scratch
    sends, gets = rest[:STEPS], rest[STEPS : 2 * STEPS]
    gather, sq_acc, sq_all, bsem, ssem, tosem, cameem, sendsem, getsem, agsend, agget, oversend, overget, sqs, sqg, outsem = rest[2 * STEPS :]
    weights, slots = 6, 2
    half_width = sum(n for _, n in chunks)
    length = half_width // slots
    shard = acc.shape[4]
    d = sdbuf.shape[1]
    me = lax.axis_index("dp")
    core, first, second = place(me, side)
    sibling = me + 1 - 2 * core
    slot_bits = [stream_bits(first, second, j) for j in range(slots)]
    partner = [[stream_partner(core, first, second, j, k, side) for k in range(STEPS)] for j in range(slots)]

    barrier = pltpu.get_barrier_semaphore()

    def greet(i, _):
        pl.semaphore_signal(barrier, inc=1, device_id={"dp": (me + i) % devices}, device_id_type=pl.DeviceIdType.MESH)

    lax.fori_loop(1, devices, greet, None)
    pl.semaphore_wait(barrier, devices - 1)

    def remote(src, dst, send, get, device_index):
        return pltpu.make_async_remote_copy(
            src_ref=src, dst_ref=dst, send_sem=send, recv_sem=get, device_id={"dp": device_index}, device_id_type=pl.DeviceIdType.MESH
        )

    def across(w):
        return remote(to, came.at[w % 2], tosem, cameem.at[w % 2], sibling)

    def hop(w, k, j):
        return remote(sends[k].at[j], gets[k].at[w % 2, j], sendsem.at[k, j], getsem.at[w % 2, k, j], partner[j][k])

    def half(bit):
        return pl.ds(2 * bit, 2)

    def spot(j, k, flip):
        b = slot_bits[j]
        bit = 1 - b[k] if flip else b[k]
        if k == 0:
            return slice(None), half(bit)
        if k == 1:
            return slice(None), 2 * b[0] + bit
        return (half(bit) if k == 2 else 2 * b[2] + bit), 2 * b[0] + b[1]

    def give(w, j, k, arrived):
        bit = slot_bits[j][k]
        going, staying = spot(j, k, True), spot(j, k, False)
        sends[k][j] = (acc[(w % 3, j, *going)] + arrived(1 - bit).astype(F32)).astype(BF16)
        hop(w, k, j).start()
        acc[(w % 3, j, *staying)] += arrived(bit).astype(F32)

    def event0(w):
        to[...] = acc[3].astype(BF16)
        across(w).start()

    def event1(w):
        across(w).wait()
        for j in range(slots):
            give(w, j, 0, lambda bit, j=j: came[w % 2, j, :, half(bit)])

    def event2(w):
        for j in range(slots):
            hop(w, 0, j).wait()
            give(w, j, 1, lambda bit, j=j: gets[0][w % 2, j, :, bit])

    def event3(w):
        for j in range(slots):
            hop(w, 1, j).wait()
            give(w, j, 2, lambda bit, j=j: gets[1][w % 2, j, half(bit)])

    def event4(w):
        for j in range(slots):
            hop(w, 2, j).wait()
            give(w, j, 3, lambda bit, j=j: gets[2][w % 2, j, bit])

    def event5(w):
        for j in range(slots):
            hop(w, 3, j).wait()
            b = slot_bits[j]
            total = acc[w % 3, j, 2 * b[2] + b[3], 2 * b[0] + b[1]] + gets[3][w % 2, j].astype(F32)
            total = total.astype(BF16)
            gather[j, 2 * b[0] + b[1], w] = total
            wide = total.astype(F32)
            sq_acc[...] += jnp.sum((wide * wide).reshape(-1, 8, LANES), axis=0)

    def fetch(t, q):
        at, n = chunks[q]
        w = t // 2
        side_of = (1 - core) * (1 - t % 2) + core * (t % 2)
        col = pl.ds(pl.multiple_of(side_of * half_width + at, LANES), n)
        buf = (len(chunks) * t + q) % 2
        return lambda src: pltpu.make_async_copy(src.at[:, col], bbuf.at[buf, :, pl.ds(0, n)], bsem.at[buf])

    def fetch_start(t, q):
        w = t // 2

        @pl.when(w % 3 == 0)
        def _():
            fetch(t, q)(hid.at[w // 3]).start()

        @pl.when(w % 3 != 0)
        def _():
            fetch(t, q)(dgu.at[w // 3, w % 3 - 1]).start()

    def fetch_small(which, layer):
        return pltpu.make_async_copy((sd, sa)[which].at[layer], (sdbuf, sabuf)[which], ssem.at[which])

    over_tokens = (((0,), (0,)), ((), ()))

    def product_down(t, q):
        at, n = chunks[q]
        value = lax.dot_general(bbuf[(len(chunks) * t + q) % 2, :, :n], sdbuf[...], over_tokens, preferred_element_type=F32)
        high, wide = length // (side * side), d // LANES
        index = (t // 2 % 3) * (t % 2) + 3 * (1 - t % 2)
        for j in range(slots):
            for b in range(side * side):
                lo, hi = max(at, j * length + b * high), min(at + n, j * length + (b + 1) * high)
                if lo < hi:
                    skip = lo - j * length - b * high
                    for c in range(wide):
                        into = c * high + skip
                        acc[index, j, b // side, b % side, into : into + hi - lo, :] = value[lo - at : hi - at, c * LANES : (c + 1) * LANES]

    def product_up(t, q):
        at, n = chunks[q]
        value = lax.dot_general(sabuf[...], bbuf[(len(chunks) * t + q) % 2, :, :n], over_tokens, preferred_element_type=F32)
        high = d // (side * side)
        index = (t // 2 % 3) * (t % 2) + 3 * (1 - t % 2)
        for col in range(at, at + n, LANES):
            j, c = col // length, col % length // LANES
            for b in range(side * side):
                acc[index, j, b // side, b % side, c * high : (c + 1) * high, :] = value[b * high : (b + 1) * high, col - at : col - at + LANES]

    sq_acc[...] = jnp.zeros_like(sq_acc)
    fetch_small(0, 0).start()
    fetch_start(0, 0)
    fetch_small(1, 0).start()

    groups = ((0, weights - 2), (weights - 2, 1), (weights - 1, 1))

    def pass_on(step, j, group):
        b, (w, n) = slot_bits[j], groups[group]
        at = 2 * b[0] + b[1] if step == 0 else 2 * b[0]
        ref = gather.at[j, pl.ds(at, 1 + step), pl.ds(w, n)]
        return remote(ref, ref, agsend.at[group, step, j], agget.at[group, step, j], partner[j][1 - step])

    def over(step, j, group):
        b, (w, n) = slot_bits[j], groups[group]
        at = pl.ds(2 * (b[0] if step == 0 else 1 - b[0]), 2)
        src, dst = gather.at[j, at, pl.ds(w, n)], (sib0, sib1)[j].at[at, pl.ds(w, n)]
        return remote(src, dst, oversend.at[group, step, j], overget.at[group, step, j], sibling)

    def out(j, group):
        w, n = groups[group]
        return pltpu.make_async_copy(gather.at[j, :, pl.ds(w, n)], (own0, own1)[j].at[:, pl.ds(w, n)], outsem.at[group, j])

    def gather_first(group):
        for j in range(slots):
            pass_on(0, j, group).start()

    def gather_second(group):
        for j in range(slots):
            pass_on(0, j, group).wait()
            pass_on(1, j, group).start()
            over(0, j, group).start()

    def gather_last(group):
        for j in range(slots):
            pass_on(1, j, group).wait()
            over(1, j, group).start()
            out(j, group).start()

    def turn(t, _):
        w, half = t // 2, t % 2

        @pl.when(t < 2 * weights)
        def _():
            for which in range(2):

                @pl.when(((w % 3 == which) & (half == 0)))
                def _():
                    fetch_small(which, w // 3).wait()

            for q in range(len(chunks)):
                fetch(t, q)(hid.at[0]).wait()
                if q + 1 < len(chunks):
                    fetch_start(t, q + 1)
                else:
                    pl.when(t + 1 < 2 * weights)(lambda: fetch_start(t + 1, 0))
                pl.when(w % 3 == 0)(lambda: product_down(t, q))
                pl.when(w % 3 != 0)(lambda: product_up(t, q))
            for which, after in ((0, 0), (1, 2)):

                @pl.when((w % 3 == after) & (half == 1) & (w < 3))
                def _():
                    fetch_small(which, 1).start()

        def at(event, back):
            pl.when((w >= back) & (w - back < weights))(lambda: event(w - back))

        @pl.when(half == 0)
        def _():
            at(event5, 3)
            at(event3, 2)
            at(event0, 0)

        @pl.when(half == 1)
        def _():
            at(event4, 2)
            at(event2, 1)
            at(event1, 0)

        pl.when(t == 2 * weights)(lambda: gather_first(0))
        pl.when(t == 2 * weights + 1)(lambda: gather_second(0))
        pl.when(t == 2 * weights + 2)(lambda: gather_first(1))

        @pl.when(t == 2 * weights + 3)
        def _():
            gather_second(1)
            gather_last(0)

        return 0

    lax.fori_loop(0, 2 * weights + 5, turn, 0)

    def count(i):
        return remote(sq_all.at[me], sq_all.at[me], sqs, sqg, (me + i) % devices)

    def counted(sem):
        return pltpu.make_async_copy(sq_all.at[pl.ds(0, devices - 1)], sq_all.at[pl.ds(0, devices - 1)], sem)

    sq_all[me] = sq_acc[...]
    gather_first(2)
    lax.fori_loop(1, devices, lambda i, _: count(i).start(), None)
    gather_second(2)
    gather_last(1)
    counted(sqs).wait()
    counted(sqg).wait()
    squares[...] = jnp.sum(sq_all[...], axis=0)
    gather_last(2)
    for group in range(len(groups)):
        for j in range(slots):
            out(j, group).wait()
            for step in range(2):
                over(step, j, group).wait()


def grads_part(hid, dgu, sd, sa, side, group, collective_id=1):
    _, t, padded = hid.shape
    d = sd.shape[2]
    half, length = padded // 2, padded // STREAMS
    chunks = [(0, half)]
    whole = d * length // LANES
    shard = whole // (side * side)
    shards = (side, side, shard, LANES)
    steps = [(side, 2, shard, LANES), (side, shard, LANES), (2, shard, LANES), (shard, LANES)]
    dma = pltpu.SemaphoreType.DMA
    quarter = jax.ShapeDtypeStruct((side, 6, shard, LANES), BF16)
    hbm = pl.BlockSpec(memory_space=pl.ANY)
    return pl.pallas_call(
        functools.partial(grads_kernel, side, group, chunks),
        in_specs=[hbm] * 4,
        out_specs=[hbm] * 4 + [pl.BlockSpec(memory_space=pltpu.VMEM)],
        out_shape=[quarter] * 4 + [jax.ShapeDtypeStruct((8, LANES), F32)],
        scratch_shapes=[
            pltpu.VMEM((2, t, chunks[0][1]), BF16),
            pltpu.VMEM((t, d), BF16),
            pltpu.VMEM((t, d), BF16),
            pltpu.VMEM((4, 2, *shards), F32),
            pltpu.VMEM((2, *shards), BF16),
            pltpu.VMEM((2, 2, *shards), BF16),
            *(pltpu.VMEM((2, *s), BF16) for s in steps),
            *(pltpu.VMEM((2, 2, *s), BF16) for s in steps),
            pltpu.VMEM((2, side, 6, shard, LANES), BF16),
            pltpu.VMEM((8, LANES), F32),
            pltpu.VMEM((group, 8, LANES), F32),
            dma((2,)),
            dma((2,)),
            dma,
            dma((2,)),
            dma((STEPS, 2)),
            dma((2, STEPS, 2)),
            dma((3, 2, 2)),
            dma((3, 2, 2)),
            dma((3, 2, 2)),
            dma((3, 2, 2)),
            dma,
            dma,
            dma((3, 2)),
        ],
        compiler_params=pltpu.CompilerParams(vmem_limit_bytes=VMEM_BYTES, collective_id=collective_id, has_side_effects=True),
        cost_estimate=pl.CostEstimate(flops=12 * t * d * padded, bytes_accessed=6 * t * padded * 2, transcendentals=0),
        name="grads",
    )(hid, dgu, sd, sa)


def update_kernel(total, shards, n_gs, n_in, there, places, *refs):
    gs, squares, refs = refs[:n_gs], refs[n_gs], refs[n_gs + 1 :]
    refs = refs[:9] + refs[n_in:]
    wg, wu, wd, mg, mu, md, vg, vu, vd, nwg, nwu, nwd, nmg, nmu, nmd, nvg, nvu, nvd, wide = refs
    source = pl.program_id(0)
    for i, g in enumerate(gs):

        @pl.when(source == i)
        def _():
            wide[...] = g[...].astype(F32)

    mean = jnp.sum(squares[...], keepdims=True) * (1.0 / total)
    factor = jnp.minimum(1.0, 0.5 * lax.rsqrt(mean + 1e-30))

    def one(w, m, v, nw, nm, nv, which):
        n = m.shape[1] // shards
        for c in range(0, m.shape[2], LANES):
            at = c // LANES * n
            g = jnp.concatenate([wide[i, which, at : at + n, :] for i in range(shards)], axis=0) * factor
            here = (0, slice(None), slice(c, c + LANES))
            new_m = 0.9 * m[here] + 0.1 * g
            new_v = 0.95 * v[here] + 0.05 * g * g
            old = w[here].astype(F32)
            nm[here] = new_m
            nv[here] = new_v
            nw[here] = (old - 0.02 * (new_m * lax.rsqrt(new_v + 1e-8) + 0.1 * old)).astype(BF16)

    pl.when(there(places))(lambda: one(wd, md, vd, nwd, nmd, nvd, 0))
    one(wg, mg, vg, nwg, nmg, nvg, 1)
    one(wu, mu, vu, nwu, nmu, nvu, 2)


def update_part(call, places, gs, squares, old, so_far, parts=2):
    shards, _, shard, _ = gs[0].shape
    layers, d, ff = old[0].shape
    length = shard * shards * shards * LANES // d
    total = 3.0 * layers * d * ff

    def g_spec(i):
        def index(s, l, h, at):
            n = jnp.clip((s - i) * layers * parts + l * parts + h, 0, layers * parts - 1)
            return n % parts, n // parts, 0, 0

        return pl.BlockSpec((shards // parts, 3, shard, LANES), index)

    def up_index(s, l, h, at):
        return layers - 1 - l, at[call, 1, s] * parts + h, at[call, 0, s]

    high = length // (shards * parts)
    last = (ff - 1) // high

    def down_block(s, h, at):
        return (at[call, 0, s] * shards + at[call, 1, s]) * parts + h

    def down_index(s, l, h, at):
        return layers - 1 - l, jnp.minimum(down_block(s, h, at), last), 0

    def there(at):
        return down_block(pl.program_id(0), pl.program_id(2), at) <= last

    up_spec = pl.BlockSpec((1, d // (shards * parts), length), up_index)
    down_spec = pl.BlockSpec((1, high, d), down_index)
    nine = [up_spec, up_spec, down_spec] * 3
    hbm = pl.BlockSpec(memory_space=pl.ANY)
    n_alias = len(so_far)
    return pl.pallas_call(
        functools.partial(update_kernel, total, shards // parts, len(gs), 9 + n_alias, there),
        grid_spec=pltpu.PrefetchScalarGridSpec(
            num_scalar_prefetch=1,
            grid=(len(gs), layers, parts),
            in_specs=[*(g_spec(i) for i in range(len(gs))), pl.BlockSpec((8, LANES), lambda *_: (0, 0)), *nine, *[hbm] * n_alias],
            out_specs=nine,
            scratch_shapes=[pltpu.VMEM((shards // parts, 3, shard, LANES), F32)],
        ),
        out_shape=[jax.ShapeDtypeStruct(a.shape, a.dtype) for a in old],
        input_output_aliases={1 + len(gs) + 1 + 9 + i: i for i in range(n_alias)},
        compiler_params=pltpu.CompilerParams(vmem_limit_bytes=VMEM_BYTES),
        cost_estimate=pl.CostEstimate(flops=30 * 3 * layers * d * ff, bytes_accessed=5 * 3 * layers * d * ff, transcendentals=0),
        name="update",
    )(places, *gs, squares, *old, *so_far)


PLAN = (
    ((False, (0, 0)), (True, (0, 0))),
    ((False, (0, 1)),),
    ((True, (0, 1)), (False, (1, 0))),
    ((True, (1, 0)), (False, (1, 1))),
    ((True, (1, 1)),),
)


def solution(mesh):
    group = mesh.shape["dp"]
    side = math.isqrt(group // 2)
    assert side == 4 and 2 * side * side == group

    def pairs(slot, step):
        found = []
        for me in range(group):
            core, first, second = place(me, side)
            found.append((me, stream_partner(core, first, second, slot, step, side)))
        return found

    siblings = [(me, me + 1 - 2 * (me % 2)) for me in range(group)]

    def stand(me, theirs, flip):
        core, first, second = place(me, side)
        found = []
        for j in range(2):
            b = stream_bits(second, first, j) if theirs else stream_bits(first, second, j)
            b = [1 - bit if turned else bit for bit, turned in zip(b[2:], flip)]
            found.append((2 * (1 - core if theirs else core) + j, 2 * b[0] + b[1]))
        return found

    table = np.zeros((group, len(PLAN), 2, STREAMS), np.int32)
    for me in range(group):
        for call, parts in enumerate(PLAN):
            for at, one in enumerate(one for theirs, flip in parts for one in stand(me, theirs, flip)):
                table[me, call, :, at] = one

    def step(x, dy, *arrays):
        wg, wu, wd = arrays[:3]
        ff = wg.shape[2]
        padded = -(-ff // (STREAMS * LANES)) * STREAMS * LANES
        hid, dgu, sd, sa = tokens_part(x[0], dy[0], wg, wu, wd, padded)
        own0, own1, sib0, sib1, squares = grads_part(hid, dgu, sd, sa, side, group)

        places = jnp.asarray(table)[lax.axis_index("dp")]

        def along(arrays, step):
            return [lax.ppermute(a, "dp", pairs(j, step)) for j, a in enumerate(arrays)]

        def across(arrays):
            return [lax.ppermute(a, "dp", siblings) for a in arrays]

        def update(call, new, *gs):
            return update_part(call, places, [g for pair in gs for g in pair], squares, arrays, new)

        own, sib = [own0, own1], [sib0, sib1]
        third, fourth = along(own, 3), along(own, 2)
        new = update(0, (), own, sib)
        third, new = lax.optimization_barrier((third, new))
        fifth, third_too = along(third, 2), across(third)
        new = update(1, new, third)
        fourth, third_too, new = lax.optimization_barrier((fourth, third_too, new))
        fourth_too = across(fourth)
        new = update(2, new, third_too, fourth)
        fifth, fourth_too, new = lax.optimization_barrier((fifth, fourth_too, new))
        fifth_too = across(fifth)
        new = update(3, new, fourth_too, fifth)
        fifth_too, new = lax.optimization_barrier((fifth_too, new))
        new = update(4, new, fifth_too)
        return tuple(new)

    return jax.shard_map(
        step,
        mesh=mesh,
        in_specs=(P(("rep", "dp"), None, None),) * 2 + (P(None, None, None),) * 9,
        out_specs=(P("rep", None, None),) * 9,
        check_vma=False,
    )
```

```python
import functools
import math

import jax
import jax.numpy as jnp
from jax import lax
from jax.experimental import pallas as pl
from jax.experimental.pallas import tpu as pltpu
from jax.sharding import PartitionSpec as P


F32, BF16 = jnp.float32, jnp.bfloat16
LANES = 128
VMEM_BYTES = 67_043_328
STREAMS = 4
STEPS = 4


def cut(n, size):
    return [(at, min(size, n - at)) for at in range(0, n, size)]


def normed(h):
    wide = h.astype(F32)
    scale = lax.rsqrt(jnp.mean(wide * wide, -1, keepdims=True) + 1e-6)
    return wide, scale


def gated(gate, up):
    sig = 0.5 * jnp.tanh(0.5 * gate) + 0.5
    silu = gate * sig
    return silu, up * (sig + silu * (1.0 - sig))


def dot(a, b):
    return jnp.dot(a, b, preferred_element_type=F32)


def dot_t(a, b):
    return lax.dot_general(a, b, (((1,), (1,)), ((), ())), preferred_element_type=F32)


def tokens_kernel(width, x_ref, dy_ref, wg_ref, wu_ref, wd_ref, hid, dgu, sd, sa, silu_ref, slope_ref):
    ff, padded = wg_ref.shape[2], hid.shape[2]
    columns = [slice(at, at + n) for at, n in cut(ff, width)]
    hid[:, :, ff:] = jnp.zeros((2, hid.shape[1], padded - ff), BF16)
    dgu[:, :, :, ff:] = jnp.zeros((2, 2, hid.shape[1], padded - ff), BF16)
    h = x_ref[...]
    wide, scale = normed(h)
    a = (wide * scale).astype(BF16)
    sa[1] = a
    for c in columns:
        gate, up = dot(a, wg_ref[0, :, c]), dot(a, wu_ref[0, :, c])
        silu, slope = gated(gate, up)
        hid[1, :, c] = (silu * up).astype(BF16)
        silu_ref[:, c] = silu
        slope_ref[:, c] = slope
    h = h + dot(hid[1, :, :ff], wd_ref[0]).astype(BF16)
    wide, scale = normed(h)
    a = (wide * scale).astype(BF16)
    sa[0] = a
    dy = dy_ref[...]
    sd[0] = dy
    for c in columns:
        gate, up = dot(a, wg_ref[1, :, c]), dot(a, wu_ref[1, :, c])
        silu, slope = gated(gate, up)
        hid[0, :, c] = (silu * up).astype(BF16)
        by_hid = dot_t(dy, wd_ref[1, c, :]).astype(BF16).astype(F32)
        dgu[0, 0, :, c] = (by_hid * slope).astype(BF16)
        dgu[0, 1, :, c] = (by_hid * silu).astype(BF16)
    by_a = dot_t(wg_ref[1], dgu[0, 0, :, :ff]).astype(BF16) + dot_t(wu_ref[1], dgu[0, 1, :, :ff]).astype(BF16)
    by_a = by_a.astype(F32).T
    along = jnp.sum(by_a * wide, -1, keepdims=True) * (1.0 / wide.shape[-1])
    by_h = dy + (scale * by_a - (scale * scale * scale * along) * wide).astype(BF16)
    sd[1] = by_h
    for c in columns:
        by_hid = dot_t(by_h, wd_ref[0, c, :]).astype(BF16).astype(F32)
        dgu[1, 0, :, c] = (by_hid * slope_ref[:, c]).astype(BF16)
        dgu[1, 1, :, c] = (by_hid * silu_ref[:, c]).astype(BF16)


def tokens_part(x, dy, wg, wu, wd, padded, rows=256, width=256):
    t, d = x.shape
    ff = wg.shape[2]
    tok = pl.BlockSpec((rows, d), lambda i: (i, 0))
    whole = lambda w: pl.BlockSpec(w.shape, lambda i: (0, 0, 0), pipeline_mode=pl.Buffered(1))
    out = lambda n: pl.BlockSpec((2, rows, n), lambda i: (0, i, 0))
    return pl.pallas_call(
        functools.partial(tokens_kernel, width),
        grid=(t // rows,),
        in_specs=[tok, tok, whole(wg), whole(wu), whole(wd)],
        out_specs=[out(padded), pl.BlockSpec((2, 2, rows, padded), lambda i: (0, 0, i, 0)), out(d), out(d)],
        out_shape=[
            jax.ShapeDtypeStruct((2, t, padded), BF16),
            jax.ShapeDtypeStruct((2, 2, t, padded), BF16),
            *[jax.ShapeDtypeStruct((2, t, d), BF16)] * 2,
        ],
        scratch_shapes=[pltpu.VMEM((rows, ff), F32)] * 2,
        compiler_params=pltpu.CompilerParams(vmem_limit_bytes=VMEM_BYTES),
        cost_estimate=pl.CostEstimate(flops=18 * t * d * ff, bytes_accessed=20 * t * ff, transcendentals=2 * t * ff),
        name="tokens",
    )(x, dy, wg, wu, wd)


def bits(p):
    return (p + p // 2) % 2, p // 2


def other(p, which):
    return p + 1 - 2 * (p % 2) if which == 0 else 3 - p


def place(me, side):
    core, chip = me % 2, me // 2
    x, y = chip // side, chip % side
    return core, x + core * (y - x), y + core * (x - y)


def device(core, first, second, side):
    x, y = first + core * (second - first), second + core * (first - second)
    return (x * side + y) * 2 + core


def stream_bits(first, second, slot):
    f, s = bits(first), bits(second)
    return (f[slot], f[1 - slot], s[slot], s[1 - slot])


def stream_partner(core, first, second, slot, step, side):
    which = slot if step % 2 == 0 else 1 - slot
    if step < 2:
        return device(core, other(first, which), second, side)
    return device(core, first, other(second, which), side)


def grads_kernel(side, devices, chunks, hid, dgu, sd, sa, own0, own1, sib0, sib1, squares, *scratch):
    bbuf, sdbuf, sabuf, acc, to, came, *rest = scratch
    sends, gets = rest[:STEPS], rest[STEPS : 2 * STEPS]
    last, gather, sq_acc, sq_all, bsem, ssem, tosem, cameem, sendsem, getsem, agsend, agget, oversend, overget, sqs, sqg, outsem = rest[2 * STEPS :]
    weights, slots = 6, 2
    half_width = sum(n for _, n in chunks)
    length = half_width // slots
    shard = acc.shape[4]
    d = sdbuf.shape[1]
    me = lax.axis_index("dp")
    core, first, second = place(me, side)
    sibling = me + 1 - 2 * core
    slot_bits = [stream_bits(first, second, j) for j in range(slots)]
    partner = [[stream_partner(core, first, second, j, k, side) for k in range(STEPS)] for j in range(slots)]

    barrier = pltpu.get_barrier_semaphore()

    def greet(i, _):
        pl.semaphore_signal(barrier, inc=1, device_id={"dp": (me + i) % devices}, device_id_type=pl.DeviceIdType.MESH)

    lax.fori_loop(1, devices, greet, None)
    pl.semaphore_wait(barrier, devices - 1)

    def remote(src, dst, send, get, device_index):
        return pltpu.make_async_remote_copy(
            src_ref=src, dst_ref=dst, send_sem=send, recv_sem=get, device_id={"dp": device_index}, device_id_type=pl.DeviceIdType.MESH
        )

    def across(w):
        return remote(to, came.at[w % 2], tosem, cameem.at[w % 2], sibling)

    def hop(w, k, j):
        return remote(sends[k].at[j], gets[k].at[w % 2, j], sendsem.at[k, j], getsem.at[w % 2, k, j], partner[j][k])

    def half(bit):
        return pl.ds(2 * bit, 2)

    def spot(j, k, flip):
        b = slot_bits[j]
        bit = 1 - b[k] if flip else b[k]
        if k == 0:
            return slice(None), half(bit)
        if k == 1:
            return slice(None), 2 * b[0] + bit
        return (half(bit) if k == 2 else 2 * b[2] + bit), 2 * b[0] + b[1]

    def give(w, j, k, arrived):
        bit = slot_bits[j][k]
        going, staying = spot(j, k, True), spot(j, k, False)
        sends[k][j] = (acc[(w % 3, j, *going)] + arrived(1 - bit).astype(F32)).astype(BF16)
        hop(w, k, j).start()
        if k == STEPS - 1:
            last[j] = acc[(w % 3, j, *staying)] + arrived(bit).astype(F32)
        else:
            acc[(w % 3, j, *staying)] += arrived(bit).astype(F32)

    def event0(w):
        to[...] = acc[3].astype(BF16)
        across(w).start()

    def event1(w):
        across(w).wait()
        for j in range(slots):
            give(w, j, 0, lambda bit, j=j: came[w % 2, j, :, half(bit)])

    def event2(w):
        for j in range(slots):
            hop(w, 0, j).wait()
            give(w, j, 1, lambda bit, j=j: gets[0][w % 2, j, :, bit])

    def event3(w):
        for j in range(slots):
            hop(w, 1, j).wait()
            give(w, j, 2, lambda bit, j=j: gets[1][w % 2, j, half(bit)])

    def event4(w):
        for j in range(slots):
            hop(w, 2, j).wait()
            give(w, j, 3, lambda bit, j=j: gets[2][w % 2, j, bit])

    def event5(w):
        for j in range(slots):
            hop(w, 3, j).wait()
            b = slot_bits[j]
            total = last[j] + gets[3][w % 2, j].astype(F32)
            total = total.astype(BF16)
            gather[j, 2 * b[0] + b[1], w] = total
            wide = total.astype(F32)
            sq_acc[...] += jnp.sum((wide * wide).reshape(-1, 8, LANES), axis=0)

    def fetch(t, q):
        at, n = chunks[q]
        w = t // 2
        side_of = (1 - core) * (1 - t % 2) + core * (t % 2)
        col = pl.ds(pl.multiple_of(side_of * half_width + at, LANES), n)
        buf = (len(chunks) * t + q) % 2
        return lambda src: pltpu.make_async_copy(src.at[:, col], bbuf.at[buf, :, pl.ds(0, n)], bsem.at[buf])

    def fetch_start(t, q):
        w = t // 2

        @pl.when(w % 3 == 0)
        def _():
            fetch(t, q)(hid.at[w // 3]).start()

        @pl.when(w % 3 != 0)
        def _():
            fetch(t, q)(dgu.at[w // 3, w % 3 - 1]).start()

    def fetch_small(which, layer):
        return pltpu.make_async_copy((sd, sa)[which].at[layer], (sdbuf, sabuf)[which], ssem.at[which])

    over_tokens = (((0,), (0,)), ((), ()))

    def product_down(t, q):
        at, n = chunks[q]
        value = lax.dot_general(bbuf[(len(chunks) * t + q) % 2, :, :n], sdbuf[...], over_tokens, preferred_element_type=F32)
        high, wide = length // (side * side), d // LANES
        index = (t // 2 % 3) * (t % 2) + 3 * (1 - t % 2)
        for j in range(slots):
            for b in range(side * side):
                lo, hi = max(at, j * length + b * high), min(at + n, j * length + (b + 1) * high)
                if lo < hi:
                    skip = lo - j * length - b * high
                    for c in range(wide):
                        into = c * high + skip
                        acc[index, j, b // side, b % side, into : into + hi - lo, :] = value[lo - at : hi - at, c * LANES : (c + 1) * LANES]

    def product_up(t, q):
        at, n = chunks[q]
        value = lax.dot_general(sabuf[...], bbuf[(len(chunks) * t + q) % 2, :, :n], over_tokens, preferred_element_type=F32)
        high = d // (side * side)
        index = (t // 2 % 3) * (t % 2) + 3 * (1 - t % 2)
        for col in range(at, at + n, LANES):
            j, c = col // length, col % length // LANES
            for b in range(side * side):
                acc[index, j, b // side, b % side, c * high : (c + 1) * high, :] = value[b * high : (b + 1) * high, col - at : col - at + LANES]

    sq_acc[...] = jnp.zeros_like(sq_acc)
    fetch_small(0, 0).start()
    fetch_start(0, 0)
    fetch_small(1, 0).start()

    groups = ((0, weights - 2), (weights - 2, 1), (weights - 1, 1))

    def pass_on(step, j, group):
        b, (w, n) = slot_bits[j], groups[group]
        at = 2 * b[0] + b[1] if step == 0 else 2 * b[0]
        ref = gather.at[j, pl.ds(at, 1 + step), pl.ds(w, n)]
        return remote(ref, ref, agsend.at[group, step, j], agget.at[group, step, j], partner[j][1 - step])

    def over(step, j, group):
        b, (w, n) = slot_bits[j], groups[group]
        at = pl.ds(2 * (b[0] if step == 0 else 1 - b[0]), 2)
        src, dst = gather.at[j, at, pl.ds(w, n)], (sib0, sib1)[j].at[at, pl.ds(w, n)]
        return remote(src, dst, oversend.at[group, step, j], overget.at[group, step, j], sibling)

    def out(j, group):
        w, n = groups[group]
        return pltpu.make_async_copy(gather.at[j, :, pl.ds(w, n)], (own0, own1)[j].at[:, pl.ds(w, n)], outsem.at[group, j])

    def gather_first(group):
        for j in range(slots):
            pass_on(0, j, group).start()

    def gather_second(group):
        for j in range(slots):
            pass_on(0, j, group).wait()
            pass_on(1, j, group).start()
            over(0, j, group).start()

    def gather_last(group):
        for j in range(slots):
            pass_on(1, j, group).wait()
            over(1, j, group).start()
            out(j, group).start()

    def turn(t, _):
        w, half = t // 2, t % 2

        @pl.when(t < 2 * weights)
        def _():
            for which in range(2):

                @pl.when(((w % 3 == which) & (half == 0)))
                def _():
                    fetch_small(which, w // 3).wait()

            for q in range(len(chunks)):
                fetch(t, q)(hid.at[0]).wait()
                if q + 1 < len(chunks):
                    fetch_start(t, q + 1)
                else:
                    pl.when(t + 1 < 2 * weights)(lambda: fetch_start(t + 1, 0))
                pl.when(w % 3 == 0)(lambda: product_down(t, q))
                pl.when(w % 3 != 0)(lambda: product_up(t, q))
            for which, after in ((0, 0), (1, 2)):

                @pl.when((w % 3 == after) & (half == 1) & (w < 3))
                def _():
                    fetch_small(which, 1).start()

        def at(event, back):
            pl.when((w >= back) & (w - back < weights))(lambda: event(w - back))

        @pl.when(half == 0)
        def _():
            at(event4, 3)
            at(event0, 0)

        pl.when(t == 2 * weights + 2)(lambda: gather_second(0))

        @pl.when(t == 2 * weights + 4)
        def _():
            gather_second(1)
            gather_last(0)

        @pl.when(half == 1)
        def _():
            at(event5, 3)
            pl.when(t == 2 * weights + 1)(lambda: gather_first(0))
            pl.when(t == 2 * weights + 3)(lambda: gather_first(1))
            at(event3, 2)
            at(event2, 1)
            at(event1, 0)

        return 0

    lax.fori_loop(0, 2 * weights + 6, turn, 0)

    def count(i):
        return remote(sq_all.at[me], sq_all.at[me], sqs, sqg, (me + i) % devices)

    def counted(sem):
        return pltpu.make_async_copy(sq_all.at[pl.ds(0, devices - 1)], sq_all.at[pl.ds(0, devices - 1)], sem)

    sq_all[me] = sq_acc[...]
    gather_first(2)
    lax.fori_loop(1, devices, lambda i, _: count(i).start(), None)
    gather_second(2)
    gather_last(1)
    counted(sqs).wait()
    counted(sqg).wait()
    squares[...] = jnp.sum(sq_all[...], axis=0)
    gather_last(2)
    for group in range(len(groups)):
        for j in range(slots):
            out(j, group).wait()
            for step in range(2):
                over(step, j, group).wait()


def grads_part(hid, dgu, sd, sa, side, group, collective_id=1):
    _, t, padded = hid.shape
    d = sd.shape[2]
    half, length = padded // 2, padded // STREAMS
    chunks = [(0, half)]
    whole = d * length // LANES
    shard = whole // (side * side)
    shards = (side, side, shard, LANES)
    steps = [(side, 2, shard, LANES), (side, shard, LANES), (2, shard, LANES), (shard, LANES)]
    dma = pltpu.SemaphoreType.DMA
    quarter = jax.ShapeDtypeStruct((side, 6, shard, LANES), BF16)
    hbm = pl.BlockSpec(memory_space=pl.ANY)
    return pl.pallas_call(
        functools.partial(grads_kernel, side, group, chunks),
        in_specs=[hbm] * 4,
        out_specs=[hbm] * 4 + [pl.BlockSpec(memory_space=pltpu.VMEM)],
        out_shape=[quarter] * 4 + [jax.ShapeDtypeStruct((8, LANES), F32)],
        scratch_shapes=[
            pltpu.VMEM((2, t, chunks[0][1]), BF16),
            pltpu.VMEM((t, d), BF16),
            pltpu.VMEM((t, d), BF16),
            pltpu.VMEM((4, 2, *shards), F32),
            pltpu.VMEM((2, *shards), BF16),
            pltpu.VMEM((2, 2, *shards), BF16),
            *(pltpu.VMEM((2, *s), BF16) for s in steps),
            *(pltpu.VMEM((2, 2, *s), BF16) for s in steps),
            pltpu.VMEM((2, shard, LANES), F32),
            pltpu.VMEM((2, side, 6, shard, LANES), BF16),
            pltpu.VMEM((8, LANES), F32),
            pltpu.VMEM((group, 8, LANES), F32),
            dma((2,)),
            dma((2,)),
            dma,
            dma((2,)),
            dma((STEPS, 2)),
            dma((2, STEPS, 2)),
            dma((3, 2, 2)),
            dma((3, 2, 2)),
            dma((3, 2, 2)),
            dma((3, 2, 2)),
            dma,
            dma,
            dma((3, 2)),
        ],
        compiler_params=pltpu.CompilerParams(vmem_limit_bytes=VMEM_BYTES, collective_id=collective_id, has_side_effects=True),
        cost_estimate=pl.CostEstimate(flops=12 * t * d * padded, bytes_accessed=6 * t * padded * 2, transcendentals=0),
        name="grads",
    )(hid, dgu, sd, sa)


PLAN = (
    ((False, (0, 0)), (True, (0, 0))),
    ((False, (0, 1)),),
    ((True, (0, 1)), (False, (1, 0))),
    ((True, (1, 0)), (False, (1, 1))),
    ((True, (1, 1)),),
)


def stand(side, theirs, flip):
    core, first, second = place(lax.axis_index("dp"), side)
    found = []
    for j in range(2):
        b = stream_bits(second, first, j) if theirs else stream_bits(first, second, j)
        b = [1 - bit if turned else bit for bit, turned in zip(b[2:], flip)]
        found.append((2 * (1 - core if theirs else core) + j, 2 * b[0] + b[1]))
    return found


def update_block(factor, there, squares, source, n_gs, wide, *refs):
    gs = refs[:n_gs]
    wg, wu, wd, mg, mu, md, vg, vu, vd, nwg, nwu, nwd, nmg, nmu, nmd, nvg, nvu, nvd = refs[n_gs:]
    shards = wide.shape[0]
    for i, g in enumerate(gs):

        @pl.when(source == i)
        def _():
            wide[...] = g[...].astype(F32)

    def one(w, m, v, nw, nm, nv, which):
        n = m.shape[1] // shards
        for c in range(0, m.shape[2], LANES):
            at = c // LANES * n
            g = jnp.concatenate([wide[i, which, at : at + n, :] for i in range(shards)], axis=0) * factor
            here = (0, slice(None), slice(c, c + LANES))
            new_m = 0.9 * m[here] + 0.1 * g
            new_v = 0.95 * v[here] + 0.05 * g * g
            old = w[here].astype(F32)
            nm[here] = new_m
            nv[here] = new_v
            nw[here] = (old - 0.02 * (new_m * lax.rsqrt(new_v + 1e-8) + 0.1 * old)).astype(BF16)

    pl.when(there)(lambda: one(wd, md, vd, nwd, nmd, nvd, 0))
    one(wg, mg, vg, nwg, nmg, nvg, 1)
    one(wu, mu, vu, nwu, nmu, nvu, 2)


def update_kernel(call, side, total, parts, buffers, squares, *refs):
    *refs, wide = refs
    places = [at for theirs, flip in PLAN[call] for at in stand(side, theirs, flip)]
    n_gs = (len(refs) - 18) if call == 0 else len(refs) - 27
    gs, old, new = refs[:n_gs], refs[n_gs : n_gs + 9], refs[-9:]
    shards, _, shard, _ = gs[0].shape
    layers, d, ff = old[0].shape
    length = shard * shards * shards * LANES // d
    mean = jnp.sum(squares[...], keepdims=True) * (1.0 / total)
    factor = jnp.minimum(1.0, 0.5 * lax.rsqrt(mean + 1e-30))
    high = length // (shards * parts)
    last = (ff - 1) // high

    def g_spec(i):
        def index(s, l, h):
            n = jnp.clip((s - i) * layers * parts + l * parts + h, 0, layers * parts - 1)
            return n % parts, n // parts, 0, 0

        return pl.BlockSpec((shards // parts, 3, shard, LANES), index, pipeline_mode=pl.Buffered(buffers))

    def at(s):
        stream, quarter = places[0]
        for i, (other_stream, other_quarter) in enumerate(places[1:], 1):
            stream, quarter = jnp.where(s == i, other_stream, stream), jnp.where(s == i, other_quarter, quarter)
        return stream, quarter

    def up_index(s, l, h):
        stream, quarter = at(s)
        return layers - 1 - l, quarter * parts + h, stream

    def down_block(s, h):
        stream, quarter = at(s)
        return (stream * shards + quarter) * parts + h

    def down_index(s, l, h):
        return layers - 1 - l, jnp.minimum(down_block(s, h), last), 0

    def nine(**kw):
        up_spec = pl.BlockSpec((1, d // (shards * parts), length), up_index, **kw)
        return [up_spec, up_spec, pl.BlockSpec((1, high, d), down_index, **kw)] * 3

    def block(at, *blocks):
        s, _, h = at.index
        update_block(factor, down_block(s, h) <= last, squares, s, n_gs, wide, *blocks)

    pltpu.emit_pipeline(
        block,
        grid=(n_gs, layers, parts),
        in_specs=[*(g_spec(i) for i in range(n_gs)), *nine(pipeline_mode=pl.Buffered(buffers))],
        out_specs=nine(),
        _explicit_indices=True,
    )(*gs, *old, *new)


def update_part(call, side, gs, squares, old, so_far, parts=1, buffers=3):
    shards, _, shard, _ = gs[0].shape
    layers, d, ff = old[0].shape
    total = 3.0 * layers * d * ff
    hbm = pl.BlockSpec(memory_space=pl.ANY)
    return pl.pallas_call(
        functools.partial(update_kernel, call, side, total, parts, buffers),
        in_specs=[pl.BlockSpec(memory_space=pltpu.VMEM), *[hbm] * (len(gs) + 9 + len(so_far))],
        out_specs=[hbm] * 9,
        out_shape=[jax.ShapeDtypeStruct(a.shape, a.dtype) for a in old],
        scratch_shapes=[pltpu.VMEM((shards // parts, 3, shard, LANES), F32)],
        input_output_aliases={1 + len(gs) + 9 + i: i for i in range(len(so_far))},
        compiler_params=pltpu.CompilerParams(vmem_limit_bytes=VMEM_BYTES),
        cost_estimate=pl.CostEstimate(flops=30 * 3 * layers * d * ff, bytes_accessed=5 * 3 * layers * d * ff, transcendentals=0),
        name="update",
    )(squares, *gs, *old, *so_far)


def solution(mesh):
    group = mesh.shape["dp"]
    side = math.isqrt(group // 2)
    assert side == 4 and 2 * side * side == group

    def pairs(slot, step):
        found = []
        for me in range(group):
            core, first, second = place(me, side)
            found.append((me, stream_partner(core, first, second, slot, step, side)))
        return found

    siblings = [(me, me + 1 - 2 * (me % 2)) for me in range(group)]

    def step(x, dy, *arrays):
        wg, wu, wd = arrays[:3]
        ff = wg.shape[2]
        padded = -(-ff // (STREAMS * LANES)) * STREAMS * LANES
        hid, dgu, sd, sa = tokens_part(x[0], dy[0], wg, wu, wd, padded)
        own0, own1, sib0, sib1, squares = grads_part(hid, dgu, sd, sa, side, group)

        def along(arrays, step):
            return [lax.ppermute(a, "dp", pairs(j, step)) for j, a in enumerate(arrays)]

        def across(arrays):
            return [lax.ppermute(a, "dp", siblings) for a in arrays]

        def update(call, new, *gs):
            return update_part(call, side, [g for pair in gs for g in pair], squares, arrays, new)

        own, sib = [own0, own1], [sib0, sib1]
        third, fourth = along(own, 3), along(own, 2)
        new = update(0, (), own, sib)
        third, new = lax.optimization_barrier((third, new))
        fifth, third_too = along(third, 2), across(third)
        new = update(1, new, third)
        fourth, third_too, new = lax.optimization_barrier((fourth, third_too, new))
        fourth_too = across(fourth)
        new = update(2, new, third_too, fourth)
        fifth, fourth_too, new = lax.optimization_barrier((fifth, fourth_too, new))
        fifth_too = across(fifth)
        new = update(3, new, fourth_too, fifth)
        fifth_too, new = lax.optimization_barrier((fifth_too, new))
        new = update(4, new, fifth_too)
        return tuple(new)

    return jax.shard_map(
        step,
        mesh=mesh,
        in_specs=(P(("rep", "dp"), None, None),) * 2 + (P(None, None, None),) * 9,
        out_specs=(P("rep", None, None),) * 9,
        check_vma=False,
    )
```

```python
import functools
import math

import jax
import jax.numpy as jnp
from jax import lax
from jax.experimental import pallas as pl
from jax.experimental.pallas import tpu as pltpu
from jax.sharding import PartitionSpec as P


F32, BF16 = jnp.float32, jnp.bfloat16
LANES = 128
VMEM_BYTES = 67_043_328
STREAMS = 4
SLOTS = 2
GROUPS = 3


def cut(n, size):
    return [(at, min(size, n - at)) for at in range(0, n, size)]


def normed(h):
    wide = h.astype(F32)
    scale = lax.rsqrt(jnp.mean(wide * wide, -1, keepdims=True) + 1e-6)
    return wide, scale


def gated(gate, up):
    sig = 0.5 * jnp.tanh(0.5 * gate) + 0.5
    silu = gate * sig
    return silu, up * (sig + silu * (1.0 - sig))


def dot(a, b):
    return jnp.dot(a, b, preferred_element_type=F32)


def dot_t(a, b):
    return lax.dot_general(a, b, (((1,), (1,)), ((), ())), preferred_element_type=F32)


def tokens_kernel(width, x_ref, dy_ref, wg_ref, wu_ref, wd_ref, hid, dgu, sd, sa, silu_ref, slope_ref):
    ff, padded = wg_ref.shape[2], hid.shape[2]
    columns = [slice(at, at + n) for at, n in cut(ff, width)]
    hid[:, :, ff:] = jnp.zeros((2, hid.shape[1], padded - ff), BF16)
    dgu[:, :, :, ff:] = jnp.zeros((2, 2, hid.shape[1], padded - ff), BF16)
    h = x_ref[...]
    wide, scale = normed(h)
    a = (wide * scale).astype(BF16)
    sa[1] = a
    for c in columns:
        gate, up = dot(a, wg_ref[0, :, c]), dot(a, wu_ref[0, :, c])
        silu, slope = gated(gate, up)
        hid[1, :, c] = (silu * up).astype(BF16)
        silu_ref[:, c] = silu
        slope_ref[:, c] = slope
    h = h + dot(hid[1, :, :ff], wd_ref[0]).astype(BF16)
    early = [dot_t(dy_ref[...], wd_ref[1, c, :]).astype(BF16) for c in columns[:3]]
    wide, scale = normed(h)
    a = (wide * scale).astype(BF16)
    sa[0] = a
    dy = dy_ref[...]
    sd[0] = dy
    for number, c in enumerate(columns):
        gate, up = dot(a, wg_ref[1, :, c]), dot(a, wu_ref[1, :, c])
        silu, slope = gated(gate, up)
        hid[0, :, c] = (silu * up).astype(BF16)
        by_hid = (early[number] if number < len(early) else dot_t(dy, wd_ref[1, c, :]).astype(BF16)).astype(F32)
        dgu[0, 0, :, c] = (by_hid * slope).astype(BF16)
        dgu[0, 1, :, c] = (by_hid * silu).astype(BF16)
    by_a = dot_t(wg_ref[1], dgu[0, 0, :, :ff]).astype(BF16) + dot_t(wu_ref[1], dgu[0, 1, :, :ff]).astype(BF16)
    by_a = by_a.astype(F32).T
    along = jnp.sum(by_a * wide, -1, keepdims=True) * (1.0 / wide.shape[-1])
    by_h = dy + (scale * by_a - (scale * scale * scale * along) * wide).astype(BF16)
    sd[1] = by_h
    for c in columns:
        by_hid = dot_t(by_h, wd_ref[0, c, :]).astype(BF16).astype(F32)
        dgu[1, 0, :, c] = (by_hid * slope_ref[:, c]).astype(BF16)
        dgu[1, 1, :, c] = (by_hid * silu_ref[:, c]).astype(BF16)


def tokens_part(x, dy, wg, wu, wd, padded, rows=256, width=256):
    t, d = x.shape
    ff = wg.shape[2]
    tok = pl.BlockSpec((rows, d), lambda i: (i, 0))
    whole = lambda w: pl.BlockSpec(w.shape, lambda i: (0, 0, 0), pipeline_mode=pl.Buffered(1))
    out = lambda n: pl.BlockSpec((2, rows, n), lambda i: (0, i, 0))
    return pl.pallas_call(
        functools.partial(tokens_kernel, width),
        grid=(t // rows,),
        in_specs=[tok, tok, whole(wg), whole(wu), whole(wd)],
        out_specs=[out(padded), pl.BlockSpec((2, 2, rows, padded), lambda i: (0, 0, i, 0)), out(d), out(d)],
        out_shape=[
            jax.ShapeDtypeStruct((2, t, padded), BF16),
            jax.ShapeDtypeStruct((2, 2, t, padded), BF16),
            *[jax.ShapeDtypeStruct((2, t, d), BF16)] * 2,
        ],
        scratch_shapes=[pltpu.VMEM((rows, ff), F32)] * 2,
        compiler_params=pltpu.CompilerParams(vmem_limit_bytes=VMEM_BYTES),
        cost_estimate=pl.CostEstimate(flops=18 * t * d * ff, bytes_accessed=20 * t * ff, transcendentals=2 * t * ff),
        name="tokens",
    )(x, dy, wg, wu, wd)


def bits(p):
    return (p + p // 2) % 2, p // 2


def other(p, which):
    return p + 1 - 2 * (p % 2) if which == 0 else 3 - p


def place(me, side):
    core, chip = me % 2, me // 2
    x, y = chip // side, chip % side
    return core, x + core * (y - x), y + core * (x - y)


def device(core, first, second, side):
    x, y = first + core * (second - first), second + core * (first - second)
    return (x * side + y) * 2 + core


def stream_bits(first, second, slot):
    f, s = bits(first), bits(second)
    return (f[slot], f[1 - slot], s[slot], s[1 - slot])


def stream_partner(core, first, second, slot, step, side):
    which = slot if step % 2 == 0 else 1 - slot
    if step < 2:
        return device(core, other(first, which), second, side)
    return device(core, first, other(second, which), side)


FLIPS = ((1, 0), (0, 1), (1, 1))


def flipped(pair, flip):
    return [1 - bit if turned else bit for bit, turned in zip(pair, flip)]


def ring_partners(core, first, second, slot, along, side):
    near = [stream_partner(core, first, second, slot, 2 * along + i, side) for i in range(2)]
    place_on = first if along == 0 else second
    far = (place_on + 2) % side
    return [*near, device(core, far, second, side) if along == 0 else device(core, first, far, side)]


def grads_kernel(side, devices, chunks, hid, dgu, sd, sa, own0, own1, sib0, sib1, squares, *scratch):
    bbuf, sdbuf, sabuf, acc, to, came, *rest = scratch
    sends, gets = rest[:3], rest[3:6]
    last, gather, sq_acc, sq_all, bsem, ssem, tosem, cameem, sendsem, getsem, free, quad, agsend, agget, oversend, overget, sqs, sqg, outsem = rest[6:]
    weights, slots = 6, 2
    half_width = sum(n for _, n in chunks)
    length = half_width // slots
    shard = acc.shape[4]
    d = sdbuf.shape[1]
    me = lax.axis_index("dp")
    core, first, second = place(me, side)
    sibling = me + 1 - 2 * core
    slot_bits = [stream_bits(first, second, j) for j in range(slots)]
    mine = [2 * b[0] + b[1] for b in slot_bits]
    partner = [[stream_partner(core, first, second, j, k, side) for k in range(2)] for j in range(slots)]
    around = [[ring_partners(core, first, second, j, axis, side) for axis in range(2)] for j in range(slots)]

    barrier = pltpu.get_barrier_semaphore()

    def greet(i, _):
        pl.semaphore_signal(barrier, inc=1, device_id={"dp": (me + i) % devices}, device_id_type=pl.DeviceIdType.MESH)

    lax.fori_loop(1, devices, greet, None)
    pl.semaphore_wait(barrier, devices - 1)

    def remote(src, dst, send, get, device_index):
        return pltpu.make_async_remote_copy(
            src_ref=src, dst_ref=dst, send_sem=send, recv_sem=get, device_id={"dp": device_index}, device_id_type=pl.DeviceIdType.MESH
        )

    def odd(w):
        return w % 2

    def across(w):
        return remote(to, came.at[odd(w)], tosem, cameem.at[odd(w)], sibling)

    def hop(w, k, j):
        return remote(sends[k].at[j], gets[k].at[odd(w), j], sendsem.at[0, k, j], getsem.at[odd(w), k, j], partner[j][k])

    def spread(w, i, j):
        return remote(
            sends[2].at[odd(w), j, i], gets[2].at[odd(w), j, i], sendsem.at[odd(w), 2 + i, j], getsem.at[odd(w), 2 + i, j], around[j][1][i]
        )

    def half(bit):
        return pl.ds(2 * bit, 2)

    def spot(j, k, flip):
        b = slot_bits[j]
        bit = 1 - b[k] if flip else b[k]
        return half(bit) if k == 0 else 2 * b[0] + bit

    def give(w, j, k, arrived):
        bit = slot_bits[j][k]
        going, staying = spot(j, k, True), spot(j, k, False)
        sends[k][j] = (acc[w % 3, j, :, going] + arrived(1 - bit).astype(F32)).astype(BF16)
        hop(w, k, j).start()
        acc[w % 3, j, :, staying] += arrived(bit).astype(F32)

    def event0(w):
        to[...] = acc[3].astype(BF16)
        across(w).start()

    def room(w, k, j):
        pl.when(w >= 1)(lambda: hop(w - 1, k, j).wait_send())
        pl.when(w >= 2)(lambda: pl.semaphore_wait(free.at[k, j], 1))

    def done(w, k, j):
        pl.when(w == weights - 1)(lambda: hop(w, k, j).wait_send())

        @pl.when(w + 2 < weights)
        def _():
            pl.semaphore_signal(free.at[k, j], inc=1, device_id={"dp": partner[j][k]}, device_id_type=pl.DeviceIdType.MESH)

    def event1(w):
        across(w).wait()
        for j in range(slots):
            room(w, 0, j)
            give(w, j, 0, lambda bit, j=j: came[odd(w), j, :, half(bit)])

    def event2(w):
        for j in range(slots):
            hop(w, 0, j).wait_recv()
            room(w, 1, j)
            give(w, j, 1, lambda bit, j=j: gets[0][odd(w), j, :, bit])
            done(w, 0, j)

    def event3(w):
        for j in range(slots):
            hop(w, 1, j).wait_recv()
            b = slot_bits[j]

            def total(pair):
                at = 2 * pair[0] + pair[1]
                return acc[w % 3, j, at, mine[j]] + gets[1][odd(w), j, at].astype(F32)

            for i, flip in enumerate(FLIPS):
                sends[2][odd(w), j, i] = total(flipped(b[2:], flip)).astype(BF16)
                pl.when(w >= 2)(lambda: pl.semaphore_wait(quad.at[i, j], 1))
                spread(w, i, j).start()
            last[odd(w), j] = total(b[2:])
            done(w, 1, j)

    def event4(w):
        for j in range(slots):
            b = slot_bits[j]
            total = last[odd(w), j]
            for i in range(len(FLIPS)):
                spread(w, i, j).wait()
                total = total + gets[2][odd(w), j, i].astype(F32)

                @pl.when(w + 2 < weights)
                def _():
                    there = {"dp": around[j][1][i]}
                    pl.semaphore_signal(quad.at[i, j], inc=1, device_id=there, device_id_type=pl.DeviceIdType.MESH)

            total = total.astype(BF16)
            gather[j, mine[j], w] = total
            wide = total.astype(F32)
            sq_acc[...] += jnp.sum((wide * wide).reshape(-1, 8, LANES), axis=0)

    def fetch(t, q):
        at, n = chunks[q]
        w = t // 2
        side_of = (1 - core) * (1 - t % 2) + core * (t % 2)
        col = pl.ds(pl.multiple_of(side_of * half_width + at, LANES), n)
        buf = (len(chunks) * t + q) % 2
        return lambda src: pltpu.make_async_copy(src.at[:, col], bbuf.at[buf, :, pl.ds(0, n)], bsem.at[buf])

    def fetch_start(t, q):
        w = t // 2

        @pl.when(w % 3 == 0)
        def _():
            fetch(t, q)(hid.at[w // 3]).start()

        @pl.when(w % 3 != 0)
        def _():
            fetch(t, q)(dgu.at[w // 3, w % 3 - 1]).start()

    def fetch_small(which, layer):
        return pltpu.make_async_copy((sd, sa)[which].at[layer], (sdbuf, sabuf)[which], ssem.at[which])

    over_tokens = (((0,), (0,)), ((), ()))

    def product_down(t, q):
        at, n = chunks[q]
        value = lax.dot_general(bbuf[(len(chunks) * t + q) % 2, :, :n], sdbuf[...], over_tokens, preferred_element_type=F32)
        high, wide = length // (side * side), d // LANES
        index = (t // 2 % 3) * (t % 2) + 3 * (1 - t % 2)
        for j in range(slots):
            for b in range(side * side):
                lo, hi = max(at, j * length + b * high), min(at + n, j * length + (b + 1) * high)
                if lo < hi:
                    skip = lo - j * length - b * high
                    for c in range(wide):
                        into = c * high + skip
                        acc[index, j, b // side, b % side, into : into + hi - lo, :] = value[lo - at : hi - at, c * LANES : (c + 1) * LANES]

    def product_up(t, q):
        at, n = chunks[q]
        value = lax.dot_general(sabuf[...], bbuf[(len(chunks) * t + q) % 2, :, :n], over_tokens, preferred_element_type=F32)
        high = d // (side * side)
        index = (t // 2 % 3) * (t % 2) + 3 * (1 - t % 2)
        for col in range(at, at + n, LANES):
            j, c = col // length, col % length // LANES
            for b in range(side * side):
                acc[index, j, b // side, b % side, c * high : (c + 1) * high, :] = value[b * high : (b + 1) * high, col - at : col - at + LANES]

    sq_acc[...] = jnp.zeros_like(sq_acc)
    fetch_small(0, 0).start()
    fetch_start(0, 0)
    fetch_small(1, 0).start()

    groups = ((0, weights - 2), (weights - 2, 1), (weights - 1, 1))

    def pass_on(i, j, group):
        b, (w, n) = slot_bits[j], groups[group]
        if group == 0:
            at, count, to_device = (mine[j], 1, partner[j][1]) if i == 0 else (2 * b[0], 2, partner[j][0])
        else:
            at, count, to_device = mine[j], 1, around[j][0][i]
        ref = gather.at[j, pl.ds(at, count), pl.ds(w, n)]
        return remote(ref, ref, agsend.at[group, i, j], agget.at[group, i, j], to_device)

    def over(i, j, group):
        b, (w, n) = slot_bits[j], groups[group]
        at = pl.ds(0, side) if group else pl.ds(2 * (b[0] if i == 0 else 1 - b[0]), 2)
        src, dst = gather.at[j, at, pl.ds(w, n)], (sib0, sib1)[j].at[at, pl.ds(w, n)]
        return remote(src, dst, oversend.at[group, i, j], overget.at[group, i, j], sibling)

    def out(j, group):
        w, n = groups[group]
        return pltpu.make_async_copy(gather.at[j, :, pl.ds(w, n)], (own0, own1)[j].at[:, pl.ds(w, n)], outsem.at[group, j])

    def gather_first(group):
        for j in range(slots):
            for i in range(len(FLIPS) if group else 1):
                pass_on(i, j, group).start()

    def gather_second():
        for j in range(slots):
            pass_on(0, j, 0).wait()
            pass_on(1, j, 0).start()
            over(0, j, 0).start()

    def gather_last(group):
        for j in range(slots):
            for i in range(len(FLIPS)) if group else (1,):
                pass_on(i, j, group).wait()
            over(0 if group else 1, j, group).start()
            out(j, group).start()

    def turn(t, _):
        w, half = t // 2, t % 2

        @pl.when(t < 2 * weights)
        def _():
            for which in range(2):

                @pl.when(((w % 3 == which) & (half == 0)))
                def _():
                    fetch_small(which, w // 3).wait()

            for q in range(len(chunks)):
                fetch(t, q)(hid.at[0]).wait()
                if q + 1 < len(chunks):
                    fetch_start(t, q + 1)
                else:
                    pl.when(t + 1 < 2 * weights)(lambda: fetch_start(t + 1, 0))
                pl.when(w % 3 == 0)(lambda: product_down(t, q))
                pl.when(w % 3 != 0)(lambda: product_up(t, q))
            for which, after in ((0, 0), (1, 2)):

                @pl.when((w % 3 == after) & (half == 1) & (w < 3))
                def _():
                    fetch_small(which, 1).start()

        def at(event, back):
            pl.when((w >= back) & (w - back < weights))(lambda: event(w - back))

        @pl.when(half == 0)
        def _():
            at(event3, 3)
            at(event4, 4)
            pl.when(t == 2 * weights + 2)(lambda: gather_first(0))
            pl.when(t == 2 * weights + 4)(lambda: gather_first(1))
            pl.when(t == 2 * weights + 4)(gather_second)
            at(event0, 0)

        @pl.when(half == 1)
        def _():
            at(event1, 0)
            at(event2, 1)

        return 0

    lax.fori_loop(0, 2 * weights + 7, turn, 0)

    def count(i):
        return remote(sq_all.at[me], sq_all.at[me], sqs, sqg, (me + i) % devices)

    def counted(sem):
        return pltpu.make_async_copy(sq_all.at[pl.ds(0, devices - 1)], sq_all.at[pl.ds(0, devices - 1)], sem)

    sq_all[me] = sq_acc[...]
    gather_first(2)
    lax.fori_loop(1, devices, lambda i, _: count(i).start(), None)
    gather_last(0)
    gather_last(1)
    gather_last(2)
    counted(sqs).wait()
    counted(sqg).wait()
    squares[...] = jnp.sum(sq_all[...], axis=0)
    for group in range(len(groups)):
        for j in range(slots):
            out(j, group).wait()
            for i in range(1 if group else 2):
                over(i, j, group).wait()


def grads_part(hid, dgu, sd, sa, side, group, collective_id=1):
    _, t, padded = hid.shape
    d = sd.shape[2]
    half, length = padded // 2, padded // STREAMS
    chunks, widest = [(0, half)], half
    whole = d * length // LANES
    shard = whole // (side * side)
    shards = (side, side, shard, LANES)
    steps = [(side, 2, shard, LANES), (side, shard, LANES), (len(FLIPS), shard, LANES)]
    dma = pltpu.SemaphoreType.DMA
    quarter = jax.ShapeDtypeStruct((side, 6, shard, LANES), BF16)
    hbm = pl.BlockSpec(memory_space=pl.ANY)
    return pl.pallas_call(
        functools.partial(grads_kernel, side, group, chunks),
        in_specs=[hbm] * 4,
        out_specs=[hbm] * 4 + [pl.BlockSpec(memory_space=pltpu.VMEM)],
        out_shape=[quarter] * 4 + [jax.ShapeDtypeStruct((8, LANES), F32)],
        scratch_shapes=[
            pltpu.VMEM((SLOTS, t, widest), BF16),
            pltpu.VMEM((t, d), BF16),
            pltpu.VMEM((t, d), BF16),
            pltpu.VMEM((4, SLOTS, *shards), F32),
            pltpu.VMEM((SLOTS, *shards), BF16),
            pltpu.VMEM((SLOTS, SLOTS, *shards), BF16),
            *(pltpu.VMEM((SLOTS, *s), BF16) for s in steps[:-1]),
            pltpu.VMEM((SLOTS, SLOTS, *steps[-1]), BF16),
            *(pltpu.VMEM((SLOTS, SLOTS, *s), BF16) for s in steps),
            pltpu.VMEM((SLOTS, SLOTS, shard, LANES), F32),
            pltpu.VMEM((SLOTS, side, 6, shard, LANES), BF16),
            pltpu.VMEM((8, LANES), F32),
            pltpu.VMEM((group, 8, LANES), F32),
            dma((SLOTS,)),
            dma((SLOTS,)),
            dma,
            dma((SLOTS,)),
            dma((SLOTS, 5, SLOTS)),
            dma((SLOTS, 5, SLOTS)),
            pltpu.SemaphoreType.REGULAR((SLOTS, SLOTS)),
            pltpu.SemaphoreType.REGULAR((GROUPS, SLOTS)),
            dma((GROUPS, GROUPS, SLOTS)),
            dma((GROUPS, GROUPS, SLOTS)),
            dma((GROUPS, SLOTS, SLOTS)),
            dma((GROUPS, SLOTS, SLOTS)),
            dma,
            dma,
            dma((GROUPS, SLOTS)),
        ],
        compiler_params=pltpu.CompilerParams(vmem_limit_bytes=VMEM_BYTES, collective_id=collective_id, has_side_effects=True),
        cost_estimate=pl.CostEstimate(flops=12 * t * d * padded, bytes_accessed=6 * t * padded * 2, transcendentals=0),
        name="grads",
    )(hid, dgu, sd, sa)


PLAN = (
    ((False, (0, 0)), (True, (0, 0))),
    ((False, (0, 1)),),
    ((True, (0, 1)), (False, (1, 0))),
    ((True, (1, 0)), (False, (1, 1))),
    ((True, (1, 1)),),
)


def stand(side, theirs, flip):
    core, first, second = place(lax.axis_index("dp"), side)
    found = []
    for j in range(2):
        b = stream_bits(second, first, j) if theirs else stream_bits(first, second, j)
        b = flipped(b[2:], flip)
        found.append((2 * (1 - core if theirs else core) + j, 2 * b[0] + b[1]))
    return found


def update_block(factor, there, squares, source, n_gs, wide, *refs):
    gs = refs[:n_gs]
    wg, wu, wd, mg, mu, md, vg, vu, vd, nwg, nwu, nwd, nmg, nmu, nmd, nvg, nvu, nvd = refs[n_gs:]
    shards = wide.shape[0]
    for i, g in enumerate(gs):

        @pl.when(source == i)
        def _():
            wide[...] = g[...].astype(F32)

    def one(w, m, v, nw, nm, nv, which):
        n = m.shape[1] // shards
        for c in range(0, m.shape[2], LANES):
            at = c // LANES * n
            g = jnp.concatenate([wide[i, which, at : at + n, :] for i in range(shards)], axis=0) * factor
            here = (0, slice(None), slice(c, c + LANES))
            new_m = 0.9 * m[here] + 0.1 * g
            new_v = 0.95 * v[here] + 0.05 * g * g
            old = w[here].astype(F32)
            nm[here] = new_m
            nv[here] = new_v
            nw[here] = (old - 0.02 * (new_m * lax.rsqrt(new_v + 1e-8) + 0.1 * old)).astype(BF16)

    pl.when(there)(lambda: one(wd, md, vd, nwd, nmd, nvd, 0))
    one(wg, mg, vg, nwg, nmg, nvg, 1)
    one(wu, mu, vu, nwu, nmu, nvu, 2)


def update_kernel(call, side, total, parts, buffers, squares, *refs):
    *refs, wide = refs
    places = [at for theirs, flip in PLAN[call] for at in stand(side, theirs, flip)]
    n_gs = (len(refs) - 18) if call == 0 else len(refs) - 27
    gs, old, new = refs[:n_gs], refs[n_gs : n_gs + 9], refs[-9:]
    shards, _, shard, _ = gs[0].shape
    layers, d, ff = old[0].shape
    length = shard * shards * shards * LANES // d
    mean = jnp.sum(squares[...], keepdims=True) * (1.0 / total)
    factor = jnp.minimum(1.0, 0.5 * lax.rsqrt(mean + 1e-30))
    high = length // (shards * parts)
    last = (ff - 1) // high

    def g_spec(i):
        def index(s, l, h):
            n = jnp.clip((s - i) * layers * parts + l * parts + h, 0, layers * parts - 1)
            return n % parts, n // parts, 0, 0

        return pl.BlockSpec((shards // parts, 3, shard, LANES), index, pipeline_mode=pl.Buffered(buffers))

    def at(s):
        stream, quarter = places[0]
        for i, (other_stream, other_quarter) in enumerate(places[1:], 1):
            stream, quarter = jnp.where(s == i, other_stream, stream), jnp.where(s == i, other_quarter, quarter)
        return stream, quarter

    def up_index(s, l, h):
        stream, quarter = at(s)
        return layers - 1 - l, quarter * parts + h, stream

    def down_block(s, h):
        stream, quarter = at(s)
        return (stream * shards + quarter) * parts + h

    def down_index(s, l, h):
        return layers - 1 - l, jnp.minimum(down_block(s, h), last), 0

    def nine(**kw):
        up_spec = pl.BlockSpec((1, d // (shards * parts), length), up_index, **kw)
        return [up_spec, up_spec, pl.BlockSpec((1, high, d), down_index, **kw)] * 3

    def block(at, *blocks):
        s, _, h = at.index
        update_block(factor, down_block(s, h) <= last, squares, s, n_gs, wide, *blocks)

    pltpu.emit_pipeline(
        block,
        grid=(n_gs, layers, parts),
        in_specs=[*(g_spec(i) for i in range(n_gs)), *nine(pipeline_mode=pl.Buffered(buffers))],
        out_specs=nine(),
        _explicit_indices=True,
    )(*gs, *old, *new)


def update_part(call, side, gs, squares, old, so_far, parts=1, buffers=3):
    shards, _, shard, _ = gs[0].shape
    layers, d, ff = old[0].shape
    total = 3.0 * layers * d * ff
    hbm = pl.BlockSpec(memory_space=pl.ANY)
    return pl.pallas_call(
        functools.partial(update_kernel, call, side, total, parts, buffers),
        in_specs=[pl.BlockSpec(memory_space=pltpu.VMEM), *[hbm] * (len(gs) + 9 + len(so_far))],
        out_specs=[hbm] * 9,
        out_shape=[jax.ShapeDtypeStruct(a.shape, a.dtype) for a in old],
        scratch_shapes=[pltpu.VMEM((shards // parts, 3, shard, LANES), F32)],
        input_output_aliases={1 + len(gs) + 9 + i: i for i in range(len(so_far))},
        compiler_params=pltpu.CompilerParams(vmem_limit_bytes=VMEM_BYTES),
        cost_estimate=pl.CostEstimate(flops=30 * 3 * layers * d * ff, bytes_accessed=5 * 3 * layers * d * ff, transcendentals=0),
        name="update",
    )(squares, *gs, *old, *so_far)


def solution(mesh):
    group = mesh.shape["dp"]
    side = math.isqrt(group // 2)
    assert side == 4 and 2 * side * side == group

    def pairs(slot, step):
        found = []
        for me in range(group):
            core, first, second = place(me, side)
            found.append((me, stream_partner(core, first, second, slot, step, side)))
        return found

    siblings = [(me, me + 1 - 2 * (me % 2)) for me in range(group)]

    def step(x, dy, *arrays):
        wg, wu, wd = arrays[:3]
        ff = wg.shape[2]
        padded = -(-ff // (STREAMS * LANES)) * STREAMS * LANES
        hid, dgu, sd, sa = tokens_part(x[0], dy[0], wg, wu, wd, padded)
        own0, own1, sib0, sib1, squares = grads_part(hid, dgu, sd, sa, side, group)

        def along(arrays, step):
            return [lax.ppermute(a, "dp", pairs(j, step)) for j, a in enumerate(arrays)]

        def across(arrays):
            return [lax.ppermute(a, "dp", siblings) for a in arrays]

        def update(call, new, *gs):
            return update_part(call, side, [g for pair in gs for g in pair], squares, arrays, new)

        own, sib = [own0, own1], [sib0, sib1]
        third, fourth = along(own, 3), along(own, 2)
        new = update(0, (), own, sib)
        third, new = lax.optimization_barrier((third, new))
        fifth, third_too = along(third, 2), across(third)
        new = update(1, new, third)
        fourth, third_too, new = lax.optimization_barrier((fourth, third_too, new))
        fourth_too = across(fourth)
        new = update(2, new, third_too, fourth)
        fifth, fourth_too, new = lax.optimization_barrier((fifth, fourth_too, new))
        fifth_too = across(fifth)
        new = update(3, new, fourth_too, fifth)
        fifth_too, new = lax.optimization_barrier((fifth_too, new))
        new = update(4, new, fifth_too)
        return tuple(new)

    return jax.shard_map(
        step,
        mesh=mesh,
        in_specs=(P(("rep", "dp"), None, None),) * 2 + (P(None, None, None),) * 9,
        out_specs=(P("rep", None, None),) * 9,
        check_vma=False,
    )
```
